32 devices in a mesh: gx: 8 (over z, y), gy: 4 (over x, core).
Axes of the slice: x: 2, y: 2, z: 4, core: 2. Of those that a mesh axis runs over, the one named last changes fastest.
Arguments:
- right_sides: bfloat16 [16, 16, 8, 256], P('gx', 'gy'), may hold values from -6 to 6
- leaf_order: int32 [16, 16, 256], P('gx', 'gy'), may hold values from 0 to 255, each once within a row
- leaf_basis: bfloat16 [16, 16, 64, 256], P('gx', 'gy'), may hold values from -0.375 to 0.375
- near_blocks: bfloat16 [16, 16, 256, 2304], P('gx', 'gy'), may hold values from -0.125 to 0.125
- leaf_coupling: bfloat16 [16, 16, 64, 1728], P('gx', 'gy'), may hold values from -0.15625 to 0.15625
- leaf_transfer: bfloat16 [16, 16, 64, 64], P('gx', 'gy'), may hold values from -0.5 to 0.5
- box_coupling: bfloat16 [8, 8, 64, 1728], P('gx', 'gy'), may hold values from -0.15625 to 0.15625
- box_transfer: bfloat16 [8, 8, 64, 64], P('gx', 'gy'), may hold values from -0.5 to 0.5
- coarse_coupling: bfloat16 [8, 4, 64, 512], P('gx', 'gy'), may hold values from -0.1875 to 0.1875
Outputs:
- product: float32 [16, 16, 8, 256], P('gx', 'gy')
The draws below stay inside these ranges and needn't reach their ends.
Inputs may be any that keep to these rules, and one draw needn't show every extreme that they name: In every leaf, leaf_order names each of 0 to 255 once.
All inputs are finite; a program needn't handle non-finite values.
Results may differ from the reference program's by a relative error of at most 0.0003.
Values may be sent and summed in bfloat16 or wider, within the bound.
No kernel may reach another device: no remote copies, remote signals or barrier semaphores. Data moves between devices by JAX's collectives and lax.ppermute only.
A program may use at most 128 MiB of HBM per device.

```python
import jax
import jax.numpy as jnp
import numpy as np
from jax import lax

LEAF = 256
R = 64
RHS = 8
GR = 16
GC = 16
BOX_ROWS = 8
BOX_COLS = 8
COARSE_ROWS = 4
COARSE_COLS = 4
COARSE = 16
HALF = 8
N_GX = 8
N_GY = 4


def shard_levels(key, shape, shards, least, top_value):
    factor_of, own = 1.0, jax.random.fold_in(key, 6)
    for axis_at, blocks in shards:
        steps = jnp.exp(jax.random.uniform(jax.random.fold_in(own, axis_at), (blocks,), jnp.float32, least / len(shards), top_value / len(shards)))
        factor_of = factor_of * jnp.repeat(steps, shape[axis_at] // blocks).reshape([-1 if axis == axis_at else 1 for axis in range(len(shape))])
    return factor_of


def normal_values(stream_key, dims, width, most, cuts=(), kind=jnp.bfloat16):
    entries = jax.random.normal(stream_key, dims, jnp.float32) * width
    if len(cuts) > 0:
        entries = shard_levels(stream_key, dims, cuts, -0.22, 0.18) * entries
    return jnp.clip(entries, min=-most, max=most).astype(kind)


def setup_inputs(seed: int = 0) -> dict:
    seeds = jax.random.split(jax.random.key(seed), 10)
    return {
        "right_sides": normal_values(seeds[0], (GR, GC, RHS, LEAF), 1.0, 6.0, ((0, 8), (1, 4))),
        "leaf_order": jax.vmap(lambda own: jax.random.permutation(own, LEAF))(jax.random.split(seeds[1], GR * GC)).reshape((GR, GC, LEAF)).astype(jnp.int32),
        "leaf_basis": normal_values(seeds[2], (GR, GC, R, LEAF), LEAF ** -0.5, 0.375, ((0, 8), (1, 4))),
        "near_blocks": normal_values(seeds[3], (GR, GC, LEAF, 9 * LEAF), (9 * LEAF) ** -0.5, 0.125, ((0, 8), (1, 4))),
        "leaf_coupling": normal_values(seeds[4], (GR, GC, R, 27 * R), (27 * R) ** -0.5, 0.15625, ((0, 8), (1, 4))),
        "leaf_transfer": normal_values(seeds[5], (GR, GC, R, R), (2 * R) ** -0.5, 0.5, ((0, 8), (1, 4))),
        "box_coupling": normal_values(seeds[6], (BOX_ROWS, BOX_COLS, R, 27 * R), (27 * R) ** -0.5, 0.15625, ((0, 8), (1, 4))),
        "box_transfer": normal_values(seeds[7], (BOX_ROWS, BOX_COLS, R, R), (2 * R) ** -0.5, 0.5, ((0, 8), (1, 4))),
        "coarse_coupling": normal_values(seeds[8], (N_GX, N_GY, R, HALF * R), (COARSE * R) ** -0.5, 0.1875, ((0, 8), (1, 4))),
    }


exact_mode = lax.Precision.HIGHEST


def slot_table():
    chosen_all = np.zeros((2, 2, 27), np.int32)
    for u in range(2):
        for v in range(2):
            chosen = [a * 6 + b for a in range(6) for b in range(6) if max(abs(a - 2 - u), abs(b - 2 - v)) > 1]
            chosen_all[u, v] = np.array(chosen, np.int32)
    return chosen_all


def couple(coeffs, matrices):
    grid_rows = coeffs.shape[0]
    grid_cols = coeffs.shape[1]
    padded = jnp.pad(coeffs, ((2, 2), (2, 2), (0, 0), (0, 0)))
    slots = jnp.asarray(slot_table())

    def one_row(parent):
        first_row = (2 * parent).astype(jnp.int32)
        row_band = lax.dynamic_slice_in_dim(padded, first_row, 6, 0)
        pieces = [row_band[a, b:b + grid_cols:2] for a in range(6) for b in range(6)]
        stacked = jnp.stack(pieces, 0)
        chosen = stacked[slots]
        couplings = lax.dynamic_slice_in_dim(matrices, first_row, 2, 0).astype(jnp.float32)
        couplings = couplings.reshape(2, grid_cols // 2, 2, R, 27, R)
        result = jnp.einsum('uvtqsj,uqvktj->uqvsk', chosen, couplings, precision=exact_mode)
        return result.reshape(2, grid_cols, RHS, R)

    result = lax.map(one_row, jnp.arange(grid_rows // 2, dtype=jnp.int32))
    return result.reshape(grid_rows, grid_cols, RHS, R)


def near_field(ordered, near_blocks):
    grid_rows = ordered.shape[0]
    grid_cols = ordered.shape[1]
    padded = jnp.pad(ordered, ((1, 1), (1, 1), (0, 0), (0, 0)))

    def one_row(row_index):
        row_band = lax.dynamic_slice_in_dim(padded, row_index, 3, 0)
        pieces = [row_band[1 + a, 1 + b:1 + b + grid_cols] for a in (-1, 0, 1) for b in (-1, 0, 1)]
        stacked = jnp.stack(pieces, 1).astype(jnp.float32)
        blocks = lax.dynamic_slice_in_dim(near_blocks, row_index, 1, 0)[0].astype(jnp.float32)
        blocks = blocks.reshape(grid_cols, LEAF, 9, LEAF)
        return jnp.einsum('cqsp,caqp->csa', stacked, blocks, precision=exact_mode)

    return lax.map(one_row, jnp.arange(grid_rows, dtype=jnp.int32))


def coarse_field(coarse_coeffs, coarse_coupling):
    coarse_flat = coarse_coeffs.reshape(COARSE, RHS, R)
    source = jnp.arange(COARSE, dtype=jnp.int32)
    source_row = source // COARSE_COLS
    source_col = source % COARSE_COLS
    target_col = jnp.arange(COARSE_COLS, dtype=jnp.int32)

    def one_row(coarse_row):
        couplings = lax.dynamic_slice_in_dim(coarse_coupling, (2 * coarse_row).astype(jnp.int32), 2, 0).astype(jnp.float32)
        couplings = couplings.reshape(2, COARSE_COLS, R, HALF, R).transpose(1, 2, 0, 3, 4).reshape(COARSE_COLS, R, COARSE, R)
        far_mask = (jnp.abs(source_row[None, :] - coarse_row) > 1) | (jnp.abs(source_col[None, :] - target_col[:, None]) > 1)
        masked = far_mask[:, :, None, None].astype(jnp.float32) * coarse_flat[None]
        return jnp.einsum('jktm,jtsm->jsk', couplings, masked, precision=exact_mode)

    return lax.map(one_row, jnp.arange(COARSE_ROWS, dtype=jnp.int32))


def reference(right_sides, leaf_order, leaf_basis, near_blocks, leaf_coupling, leaf_transfer, box_coupling, box_transfer, coarse_coupling):
    order_index = jnp.broadcast_to(leaf_order[:, :, None, :], right_sides.shape)
    ordered = jnp.take_along_axis(right_sides, order_index, axis=3)
    basis_wide = leaf_basis.astype(jnp.float32)
    leaf_coeffs = jnp.einsum('rcsp,rckp->rcsk', ordered.astype(jnp.float32), basis_wide, precision=exact_mode)
    grouped = leaf_coeffs.reshape(BOX_ROWS, 2, BOX_COLS, 2, RHS, R)
    leaf_up = leaf_transfer.astype(jnp.float32).reshape(BOX_ROWS, 2, BOX_COLS, 2, R, R)
    box_coeffs = jnp.einsum('iujvsk,iujvkm->ijsm', grouped, leaf_up, precision=exact_mode)
    box_up = box_transfer.astype(jnp.float32).reshape(COARSE_ROWS, 2, COARSE_COLS, 2, R, R)
    coarse_coeffs = jnp.einsum('iujvsk,iujvkm->ijsm', box_coeffs.reshape(COARSE_ROWS, 2, COARSE_COLS, 2, RHS, R), box_up, precision=exact_mode)
    coarse_far = coarse_field(coarse_coeffs, coarse_coupling)
    box_far = couple(box_coeffs, box_coupling)
    leaf_far = couple(leaf_coeffs, leaf_coupling)
    coarse_spread = jnp.repeat(jnp.repeat(coarse_far, 2, axis=0), 2, axis=1)
    box_down = jnp.einsum('ijsm,ijkm->ijsk', coarse_spread, box_transfer.astype(jnp.float32), precision=exact_mode) + box_far
    box_spread = jnp.repeat(jnp.repeat(box_down, 2, axis=0), 2, axis=1)
    leaf_down = jnp.einsum('rcsm,rckm->rcsk', box_spread, leaf_transfer.astype(jnp.float32), precision=exact_mode) + leaf_far
    values = jnp.einsum('rcsk,rckp->rcsp', leaf_down, basis_wide, precision=exact_mode) + near_field(ordered, near_blocks)
    inverse = jnp.argsort(leaf_order, axis=-1).astype(jnp.int32)
    inverse_index = jnp.broadcast_to(inverse[:, :, None, :], values.shape)
    return jnp.take_along_axis(values, inverse_index, axis=3)
```

```python
import functools

import jax
import jax.numpy as jnp
from jax import lax
from jax.experimental import pallas as pl
from jax.experimental.pallas import tpu as pltpu
from jax.sharding import PartitionSpec as P

F32 = jnp.float32
BF16 = jnp.bfloat16


def nt(a, b):
    return lax.dot_general(a, b, (((1,), (1,)), ((), ())), preferred_element_type=F32)


def nn(a, b):
    return lax.dot_general(a, b, (((1,), (0,)), ((), ())), preferred_element_type=F32)


def split(x):
    hi = x.astype(BF16).astype(F32)
    return jnp.concatenate([hi, x - hi], 0).astype(BF16)


def join(y):
    half = y.shape[0] // 2
    wide = y.astype(F32)
    return wide[:half] + wide[half:]


def fold(x):
    half = x.shape[0] // 2
    return x[:half] + x[half:]


def one_hot(order_row, n_points):
    place = lax.broadcasted_iota(jnp.int32, (n_points, n_points), 0)
    return (place == order_row).astype(F32).astype(BF16)


def slot_list(u, v):
    return [
        (a, b) for a in range(6) for b in range(6) if max(abs(a - 2 - u), abs(b - 2 - v)) > 1
    ]


def pick_slots(window, base, u, v, rank):
    lane = lax.broadcasted_iota(jnp.int32, (window.shape[1], 2 * rank), 1)
    cache = {}

    def half(a, b, side):
        key = (a, b // 2, b % 2 != side)
        if key not in cache:
            start = base + (b // 2) * 2 * rank
            value = window[a, :, start : start + 2 * rank]
            cache[key] = pltpu.roll(value, rank, 1) if key[2] else value
        return cache[key]

    slots = slot_list(u, v)
    pieces = []
    for k in range(0, len(slots), 2):
        low = slots[k]
        if k + 1 == len(slots):
            pieces.append(half(*low, 0)[:, :rank])
            continue
        high = slots[k + 1]
        left, right = half(*low, 0), half(*high, 1)
        pieces.append(left if left is right else jnp.where(lane < rank, left, right))
    return jnp.concatenate(pieces, 1)


def up_kernel(rs, order, basis, leaf_up, box_up, pts, send):
    rows, cols, n_rhs, n_points = rs.shape
    rank = basis.shape[2]
    coeff_rows = []
    for u in range(rows):
        coeff_rows.append([])
    columns = []
    for c in range(cols):
        pair = []
        for u in range(rows):
            chosen = one_hot(order[u, c : c + 1, :], n_points)
            ordered = nn(rs[u, c], chosen)
            pair.append(ordered)
            coeff_rows[u].append(nt(ordered.astype(BF16), basis[u, c]))
        column = jnp.concatenate(pair, 0).astype(BF16)
        columns.append(column)
        pts[:, c * n_points : (c + 1) * n_points] = column
    send[:, 0:n_points] = columns[0]
    send[:, n_points : 2 * n_points] = columns[-1]
    at = 2 * n_points
    wide = [jnp.concatenate(row, 1) for row in coeff_rows]
    coeffs = [split(row) for row in wide]
    for u in range(rows):
        send[:, at : at + cols * rank] = coeffs[u]
        at += cols * rank
    boxes = []
    for w in range(cols // 2):
        total = None
        for u in range(rows):
            part = nn(
                coeffs[u][:, 2 * w * rank : 2 * (w + 1) * rank],
                leaf_up[u, 2 * w : 2 * w + 2].reshape(2 * rank, rank),
            )
            total = part if total is None else total + part
        boxes.append(fold(total))
    boxes = split(jnp.concatenate(boxes, 1))
    send[:, at : at + 2 * rank] = boxes
    at += 2 * rank
    share = fold(nn(boxes, box_up[0].reshape(2 * rank, rank)))
    send[:, at : at + 2 * rank] = split(jnp.concatenate([share, share], 1))


def masked(flag, value):
    return jnp.where(flag, value.astype(F32), 0.0).astype(BF16)


def strip_kernel(n_gy, rank, n_points, cols, pts, send, gathered, out):
    here = lax.axis_index("gy")
    left = jnp.maximum(here - 1, 0)
    right = jnp.minimum(here + 1, n_gy - 1)
    has_left, has_right = here > 0, here < n_gy - 1
    out[:, 0:n_points] = masked(has_left, gathered[left, :, n_points : 2 * n_points])
    out[:, n_points : (cols + 1) * n_points] = pts[...]
    at = (cols + 2) * n_points
    out[:, at - n_points : at] = masked(has_right, gathered[right, :, 0:n_points])
    source = 2 * n_points
    width = cols * rank
    for u in range(2):
        out[:, at : at + 2 * rank] = masked(
            has_left, gathered[left, :, source + width - 2 * rank : source + width]
        )
        at += 2 * rank
        out[:, at : at + width] = send[:, source : source + width]
        at += width
        out[:, at : at + 2 * rank] = masked(
            has_right, gathered[right, :, source : source + 2 * rank]
        )
        at += 2 * rank
        source += width
    out[:, at : at + 2 * rank] = masked(has_left, gathered[left, :, source : source + 2 * rank])
    out[:, at + 2 * rank : at + 4 * rank] = send[:, source : source + 2 * rank]
    out[:, at + 4 * rank : at + 6 * rank] = masked(
        has_right, gathered[right, :, source : source + 2 * rank]
    )
    at += 6 * rank
    source += 2 * rank
    lane = lax.broadcasted_iota(jnp.int32, (send.shape[0], 2 * rank), 1)
    for k in range(n_gy // 2):
        low = gathered[2 * k, :, source : source + 2 * rank].astype(F32)
        high = gathered[2 * k + 1, :, source : source + 2 * rank].astype(F32)
        out[:, at : at + 2 * rank] = jnp.where(lane < rank, low, high).astype(BF16)
        at += 2 * rank


def near_own_kernel(n_points, mine, near, out):
    rows, cols = out.shape[0], out.shape[1]
    for u in range(rows):
        for c in range(cols):
            total = None
            for v in range(rows):
                q = 3 * (v - u + 1)
                product = nt(
                    mine[:, c * n_points : (c + 3) * n_points],
                    near[u, c, :, q * n_points : (q + 3) * n_points],
                )
                half = product[:8] if v == 0 else product[8:]
                total = half if total is None else total + half
            out[u, c] = total


def relay_kernel(n_gy, rank, n_points, cols, mine, other, halo, boxes, coarse):
    parity = lax.axis_index("gx") % 2
    even = parity == 0
    p_width = (cols + 2) * n_points
    c_width = 2 * (cols + 4) * rank
    b_width = 6 * rank
    s_width = n_gy * rank
    wide = other[:, 0:p_width].astype(F32)
    row = jnp.where(even, wide[8:], wide[:8])
    half = p_width // 2
    halo[:, 0:half] = jnp.concatenate([row[:, :half], row[:, half:]], 0).astype(BF16)
    halo[:, half : half + c_width] = other[:, p_width : p_width + c_width]
    at = p_width + c_width
    a_box = mine[:, at : at + b_width].astype(F32)
    b_box = other[:, at : at + b_width].astype(F32)
    top = jnp.where(even, a_box, b_box).astype(BF16)
    bottom = jnp.where(even, b_box, a_box).astype(BF16)
    total = split(join(mine[:, at + b_width :]) + join(other[:, at + b_width :]))
    to = half + c_width
    halo[:, to : to + b_width] = top
    halo[:, to + b_width : to + 2 * b_width] = bottom
    halo[:, to + 2 * b_width :] = total
    boxes[:, 0:b_width] = top
    boxes[:, b_width : 2 * b_width] = bottom
    boxes[:, 2 * b_width :] = total
    coarse[...] = total


def down_kernel(
    n_gx,
    n_gy,
    order,
    basis,
    near,
    leaf_coupling,
    leaf_up,
    box_coupling,
    box_up,
    coupling_mine,
    coupling_other,
    mine,
    other,
    halo,
    boxes,
    coarse,
    *rest,
):
    far_parts = rest[: n_gx // 2 - 3]
    near_own, out, leaf_window, box_window, weights = rest[n_gx // 2 - 3 :]
    rows, cols, rank, n_points = basis.shape
    n_z = n_gx // 2
    here_x = lax.axis_index("gx")
    here_y = lax.axis_index("gy")
    parity = here_x % 2
    even = parity == 0
    z = here_x // 2
    has_up, has_down = z > 0, z < n_z - 1
    p_width = (cols + 2) * n_points
    half = p_width // 2
    row_width = (cols + 4) * rank
    c_width = 2 * row_width
    b_width = 6 * rank
    s_width = n_gy * rank

    strip = halo[:, 0:half].astype(F32)
    strip = jnp.concatenate([strip[:8], strip[8:]], 1)
    partner = other[:, 0:p_width].astype(F32)
    above = jnp.where(even, jnp.where(has_up, strip, 0.0), partner[8:])
    below = jnp.where(even, partner[:8], jnp.where(has_down, strip, 0.0))
    rim = jnp.concatenate([above, below], 0).astype(BF16)

    for u in range(2):
        span = slice(half + u * row_width, half + (u + 1) * row_width)
        from_halo = join(halo[:, span])
        span = slice(p_width + u * row_width, p_width + (u + 1) * row_width)
        from_other = join(other[:, span])
        leaf_window[u] = jnp.where(even, jnp.where(has_up, from_halo, 0.0), from_other)
        leaf_window[2 + u] = join(mine[:, span])
        leaf_window[4 + u] = jnp.where(even, from_other, jnp.where(has_down, from_halo, 0.0))

    at = p_width + c_width
    a_box, b_box = join(mine[:, at : at + b_width]), join(other[:, at : at + b_width])
    box_window[2] = jnp.where(even, a_box, b_box)
    box_window[3] = jnp.where(even, b_box, a_box)
    for u in range(2):
        start = half + c_width + u * b_width
        from_halo = join(halo[:, start : start + b_width])
        from_boxes = join(boxes[:, u * b_width : (u + 1) * b_width])
        box_window[u] = jnp.where(has_up, jnp.where(even, from_halo, from_boxes), 0.0)
        box_window[4 + u] = jnp.where(has_down, jnp.where(even, from_boxes, from_halo), 0.0)

    half_width = coupling_mine.shape[-1]
    own_half = coupling_mine[0, 0]
    their_half = coupling_other[0, 0]
    first = jnp.where(even, own_half.astype(F32), their_half.astype(F32)).astype(BF16)
    second = jnp.where(even, their_half.astype(F32), own_half.astype(F32)).astype(BF16)
    weights[:, 0:half_width] = first
    weights[:, half_width:] = second
    lane = lax.broadcasted_iota(jnp.int32, (16, s_width), 1) // rank
    wide_gap = jnp.abs(lane - here_y) > 1
    start = half + c_width + 2 * b_width
    step = jnp.where(even, 1, -1)
    sources = [
        (z, coarse[...]),
        (lax.rem(z - step + n_z, n_z), halo[:, start:]),
        (lax.rem(z + step + n_z, n_z), boxes[:, 2 * b_width :]),
    ]
    for d, part in enumerate(far_parts):
        sources.append((lax.rem(z - (d + 2) + n_z, n_z), part[...]))
    coarse_far = None
    for place, value in sources:
        far = jnp.logical_or(wide_gap, jnp.abs(place - z) > 1)
        chosen = jnp.where(far, value.astype(F32), 0.0).astype(BF16)
        columns = pl.ds(pl.multiple_of(place * s_width, s_width), s_width)
        part = nt(chosen, weights[:, columns])
        coarse_far = part if coarse_far is None else coarse_far + part
    coarse_far = split(fold(coarse_far))

    box_down = []
    for v in range(cols // 2):
        listed = jnp.where(
            even,
            pick_slots(box_window, 0, 0, v, rank),
            pick_slots(box_window, 0, 1, v, rank),
        )
        value = nt(split(listed), box_coupling[0, v]) + nt(coarse_far, box_up[0, v])
        box_down.append(split(fold(value)))

    for u in range(rows):
        for c in range(cols):
            w, v = c // 2, c % 2
            listed = split(pick_slots(leaf_window, 2 * w * rank, u, v, rank))
            down = nt(listed, leaf_coupling[u, c]) + nt(box_down[w], leaf_up[u, c])
            values = fold(nn(split(fold(down)), basis[u, c]))
            q = 6 * u
            outer = nt(
                rim[:, c * n_points : (c + 3) * n_points],
                near[u, c, :, q * n_points : (q + 3) * n_points],
            )
            values = values + near_own[u, c] + (outer[:8] if u == 0 else outer[8:])
            chosen = one_hot(order[u, c : c + 1, :], n_points)
            out[u, c] = fold(nt(split(values), chosen))


def call(kernel, outs, operands, scratch=(), flops=0, name=None):
    space = pl.BlockSpec(memory_space=pltpu.VMEM)
    return pl.pallas_call(
        kernel,
        out_shape=outs,
        in_specs=[space] * len(operands),
        out_specs=jax.tree.map(lambda _: space, outs),
        scratch_shapes=list(scratch),
        cost_estimate=pl.CostEstimate(flops=flops, bytes_accessed=0, transcendentals=0),
        name=name,
    )(*operands)


def body(
    n_gx,
    n_gy,
    right_sides,
    leaf_order,
    leaf_basis,
    near_blocks,
    leaf_coupling,
    leaf_transfer,
    box_coupling,
    box_transfer,
    coarse_coupling,
):
    rows, cols, n_rhs, n_points = right_sides.shape
    rank = leaf_basis.shape[2]
    n_z = n_gx // 2
    tall = 2 * n_rhs
    shape = jax.ShapeDtypeStruct

    def move(value, pairs):
        return lax.ppermute(value, "gx", pairs)

    swap = [(i, i ^ 1) for i in range(n_gx)]

    def along(by):
        return [(i, 2 * ((i // 2 + by[i % 2]) % n_z) + i % 2) for i in range(n_gx)]

    coupling_other = move(coarse_coupling, swap)
    send_width = 2 * n_points + 2 * cols * rank + 4 * rank
    pts, send = call(
        up_kernel,
        (shape((tall, cols * n_points), BF16), shape((tall, send_width), BF16)),
        (right_sides, leaf_order, leaf_basis, leaf_transfer, box_transfer),
        name="up",
    )
    gathered = lax.all_gather(send, "gy", axis=0)
    p_width = (cols + 2) * n_points
    c_width = 2 * (cols + 4) * rank
    b_width = 6 * rank
    s_width = n_gy * rank
    mine = call(
        functools.partial(strip_kernel, n_gy, rank, n_points, cols),
        shape((tall, p_width + c_width + b_width + s_width), BF16),
        (pts, send, gathered),
        name="strip",
    )
    other = move(mine, swap)
    near_own = call(
        functools.partial(near_own_kernel, n_points),
        shape((rows, cols, n_rhs, n_points), F32),
        (mine, near_blocks),
        flops=2 * tall * 6 * rows * cols * n_points * n_points,
        name="near_own",
    )
    halo, boxes, coarse = call(
        functools.partial(relay_kernel, n_gy, rank, n_points, cols),
        (
            shape((tall, p_width // 2 + c_width + 2 * b_width + s_width), BF16),
            shape((tall, 2 * b_width + s_width), BF16),
            shape((tall, s_width), BF16),
        ),
        (mine, other),
        name="relay",
    )
    halo_in = move(halo, along((1, -1)))
    boxes_in = move(boxes, along((-1, 1)))
    far_parts = [move(coarse, along((d, d))) for d in range(2, n_z - 1)]
    return call(
        functools.partial(down_kernel, n_gx, n_gy),
        shape((rows, cols, n_rhs, n_points), F32),
        (
            leaf_order,
            leaf_basis,
            near_blocks,
            leaf_coupling,
            leaf_transfer,
            box_coupling,
            box_transfer,
            coarse_coupling,
            coupling_other,
            mine,
            other,
            halo_in,
            boxes_in,
            coarse,
            *far_parts,
            near_own,
        ),
        scratch=(
            pltpu.VMEM((6, n_rhs, (cols + 4) * rank), F32),
            pltpu.VMEM((6, n_rhs, b_width), F32),
            pltpu.VMEM((rank, n_z * s_width), BF16),
        ),
        name="down",
    )


def solution(mesh):
    spec = P("gx", "gy")
    return jax.shard_map(
        functools.partial(body, mesh.shape["gx"], mesh.shape["gy"]),
        mesh=mesh,
        in_specs=(spec,) * 9,
        out_specs=spec,
        check_vma=False,
    )
```

```python
import functools

import jax
import jax.numpy as jnp
from jax import lax
from jax.experimental import pallas as pl
from jax.experimental.pallas import tpu as pltpu
from jax.sharding import PartitionSpec as P

F32 = jnp.float32
BF16 = jnp.bfloat16


def nt(a, b):
    return lax.dot_general(a, b, (((1,), (1,)), ((), ())), preferred_element_type=F32)


def nn(a, b):
    return lax.dot_general(a, b, (((1,), (0,)), ((), ())), preferred_element_type=F32)


def split(x):
    hi = x.astype(BF16).astype(F32)
    return jnp.concatenate([hi, x - hi], 0).astype(BF16)


def join(y):
    half = y.shape[0] // 2
    wide = y.astype(F32)
    return wide[:half] + wide[half:]


def fold(x):
    half = x.shape[0] // 2
    return x[:half] + x[half:]


def one_hot(order_row, n_points):
    place = lax.broadcasted_iota(jnp.int32, (n_points, n_points), 0)
    return (place == order_row).astype(F32).astype(BF16)


def slot_list(u, v):
    return [
        (a, b) for a in range(6) for b in range(6) if max(abs(a - 2 - u), abs(b - 2 - v)) > 1
    ]


def pick_slots(window, base, u, v, rank):
    lane = lax.broadcasted_iota(jnp.int32, (window.shape[1], 2 * rank), 1)
    cache = {}

    def half(a, b, side):
        key = (a, b // 2, b % 2 != side)
        if key not in cache:
            start = base + (b // 2) * 2 * rank
            value = window[a, :, start : start + 2 * rank]
            cache[key] = pltpu.roll(value, rank, 1) if key[2] else value
        return cache[key]

    slots = slot_list(u, v)
    pieces = []
    for k in range(0, len(slots), 2):
        low = slots[k]
        if k + 1 == len(slots):
            pieces.append(half(*low, 0)[:, :rank])
            continue
        high = slots[k + 1]
        left, right = half(*low, 0), half(*high, 1)
        pieces.append(left if left is right else jnp.where(lane < rank, left, right))
    return jnp.concatenate(pieces, 1)


def up_kernel(copies, rs, order, basis, leaf_up, box_up, pts, send):
    rows, cols, n_rhs, n_points = rs.shape
    rank = basis.shape[2]
    coeff_rows = [[] for _ in range(rows)]
    copies[1].wait()
    copies[0].wait()
    copies[2].wait()
    columns = []
    for c in range(cols):
        pair = []
        for u in range(rows):
            chosen = one_hot(order[u, c : c + 1, :], n_points)
            ordered = nn(rs[u, c], chosen)
            pair.append(ordered)
            coeff_rows[u].append(nt(ordered.astype(BF16), basis[u, c]))
        column = jnp.concatenate(pair, 0).astype(BF16)
        columns.append(column)
        pts[:, c * n_points : (c + 1) * n_points] = column
    send[:, 0:n_points] = columns[0]
    send[:, n_points : 2 * n_points] = columns[-1]
    at = 2 * n_points
    wide = [jnp.concatenate(row, 1) for row in coeff_rows]
    coeffs = [split(row) for row in wide]
    for u in range(rows):
        send[:, at : at + cols * rank] = coeffs[u]
        at += cols * rank
    boxes = []
    copies[3].wait()
    copies[4].wait()
    for w in range(cols // 2):
        total = None
        for u in range(rows):
            part = nn(
                coeffs[u][:, 2 * w * rank : 2 * (w + 1) * rank],
                leaf_up[u, 2 * w : 2 * w + 2].reshape(2 * rank, rank),
            )
            total = part if total is None else total + part
        boxes.append(fold(total))
    boxes = split(jnp.concatenate(boxes, 1))
    send[:, at : at + 2 * rank] = boxes
    at += 2 * rank
    share = fold(nn(boxes, box_up[0].reshape(2 * rank, rank)))
    send[:, at : at + 2 * rank] = split(jnp.concatenate([share, share], 1))


def masked(flag, value):
    return jnp.where(flag, value.astype(F32), 0.0).astype(BF16)


def strip_kernel(n_gy, rank, n_points, cols, pts, send, gathered, out):
    here = lax.axis_index("gy")
    left = jnp.maximum(here - 1, 0)
    right = jnp.minimum(here + 1, n_gy - 1)
    has_left, has_right = here > 0, here < n_gy - 1
    out[:, 0:n_points] = masked(has_left, gathered[left, :, n_points : 2 * n_points])
    out[:, n_points : (cols + 1) * n_points] = pts[...]
    at = (cols + 2) * n_points
    out[:, at - n_points : at] = masked(has_right, gathered[right, :, 0:n_points])
    source = 2 * n_points
    width = cols * rank
    for u in range(2):
        out[:, at : at + 2 * rank] = masked(
            has_left, gathered[left, :, source + width - 2 * rank : source + width]
        )
        at += 2 * rank
        out[:, at : at + width] = send[:, source : source + width]
        at += width
        out[:, at : at + 2 * rank] = masked(
            has_right, gathered[right, :, source : source + 2 * rank]
        )
        at += 2 * rank
        source += width
    out[:, at : at + 2 * rank] = masked(has_left, gathered[left, :, source : source + 2 * rank])
    out[:, at + 2 * rank : at + 4 * rank] = send[:, source : source + 2 * rank]
    out[:, at + 4 * rank : at + 6 * rank] = masked(
        has_right, gathered[right, :, source : source + 2 * rank]
    )
    at += 6 * rank
    source += 2 * rank
    lane = lax.broadcasted_iota(jnp.int32, (send.shape[0], 2 * rank), 1)
    for k in range(n_gy // 2):
        low = gathered[2 * k, :, source : source + 2 * rank].astype(F32)
        high = gathered[2 * k + 1, :, source : source + 2 * rank].astype(F32)
        out[:, at : at + 2 * rank] = jnp.where(lane < rank, low, high).astype(BF16)
        at += 2 * rank


def near_own_kernel(n_points, mine, near, out, blocks, arrived):
    rows, cols = out.shape[0], out.shape[1]
    copies = []
    for c in range(cols):
        for u in range(rows):
            first = 3 * n_points * (1 - u)
            copies.append(
                pltpu.make_async_copy(
                    near.at[u, c, :, first : first + 6 * n_points],
                    blocks.at[u, c],
                    arrived.at[u, c],
                )
            )
            copies[-1].start()
    wide = mine[:, 0 : (cols + 2) * n_points].astype(F32)
    top, bottom = wide[:8].astype(BF16), wide[8:].astype(BF16)
    for c in range(cols):
        span = slice(c * n_points, (c + 3) * n_points)
        points = jnp.concatenate([top[:, span], bottom[:, span]], 1)
        for u in range(rows):
            copies[c * rows + u].wait()
            out[u, c] = nt(blocks[u, c], points).T


def relay_kernel(n_gy, rank, n_points, cols, mine, other, halo, boxes, coarse):
    parity = lax.axis_index("gx") % 2
    even = parity == 0
    p_width = (cols + 2) * n_points
    c_width = 2 * (cols + 4) * rank
    b_width = 6 * rank
    s_width = n_gy * rank
    wide = other[:, 0:p_width].astype(F32)
    row = jnp.where(even, wide[8:], wide[:8])
    half = p_width // 2
    halo[:, 0:half] = jnp.concatenate([row[:, :half], row[:, half:]], 0).astype(BF16)
    halo[:, half : half + c_width] = other[:, p_width : p_width + c_width]
    at = p_width + c_width
    a_box = mine[:, at : at + b_width].astype(F32)
    b_box = other[:, at : at + b_width].astype(F32)
    top = jnp.where(even, a_box, b_box).astype(BF16)
    bottom = jnp.where(even, b_box, a_box).astype(BF16)
    total = split(join(mine[:, at + b_width :]) + join(other[:, at + b_width :]))
    to = half + c_width
    halo[:, to : to + b_width] = top
    halo[:, to + b_width : to + 2 * b_width] = bottom
    halo[:, to + 2 * b_width :] = total
    boxes[:, 0:b_width] = top
    boxes[:, b_width : 2 * b_width] = bottom
    boxes[:, 2 * b_width :] = total
    coarse[...] = total


def down_kernel(
    n_gx,
    n_gy,
    order,
    basis,
    near,
    leaf_coupling,
    leaf_up,
    box_coupling,
    box_up,
    coupling_mine,
    coupling_other,
    mine,
    other,
    halo,
    boxes,
    coarse,
    *rest,
):
    far_parts = rest[: n_gx // 2 - 3]
    near_own, out, leaf_window, box_window, weights, blocks, arrived = rest[n_gx // 2 - 3 :]
    rows, cols, rank, n_points = basis.shape
    copies = {}
    for u in range(rows):
        for c in range(cols):
            first = 6 * n_points * u
            copies[u, c] = pltpu.make_async_copy(
                near.at[u, c, :, first : first + 3 * n_points],
                blocks.at[u, c],
                arrived.at[u, c],
            )
            copies[u, c].start()
    n_z = n_gx // 2
    here_x = lax.axis_index("gx")
    here_y = lax.axis_index("gy")
    parity = here_x % 2
    even = parity == 0
    z = here_x // 2
    has_up, has_down = z > 0, z < n_z - 1
    p_width = (cols + 2) * n_points
    half = p_width // 2
    row_width = (cols + 4) * rank
    c_width = 2 * row_width
    b_width = 6 * rank
    s_width = n_gy * rank

    strip = halo[:, 0:half].astype(F32)
    strip = jnp.concatenate([strip[:8], strip[8:]], 1)
    partner = other[:, 0:p_width].astype(F32)
    above = jnp.where(even, jnp.where(has_up, strip, 0.0), partner[8:])
    below = jnp.where(even, partner[:8], jnp.where(has_down, strip, 0.0))
    rim = (above.astype(BF16), below.astype(BF16))

    for u in range(2):
        span = slice(half + u * row_width, half + (u + 1) * row_width)
        from_halo = join(halo[:, span])
        span = slice(p_width + u * row_width, p_width + (u + 1) * row_width)
        from_other = join(other[:, span])
        leaf_window[u] = jnp.where(even, jnp.where(has_up, from_halo, 0.0), from_other)
        leaf_window[2 + u] = join(mine[:, span])
        leaf_window[4 + u] = jnp.where(even, from_other, jnp.where(has_down, from_halo, 0.0))

    at = p_width + c_width
    a_box, b_box = join(mine[:, at : at + b_width]), join(other[:, at : at + b_width])
    box_window[2] = jnp.where(even, a_box, b_box)
    box_window[3] = jnp.where(even, b_box, a_box)
    for u in range(2):
        start = half + c_width + u * b_width
        from_halo = join(halo[:, start : start + b_width])
        from_boxes = join(boxes[:, u * b_width : (u + 1) * b_width])
        box_window[u] = jnp.where(has_up, jnp.where(even, from_halo, from_boxes), 0.0)
        box_window[4 + u] = jnp.where(has_down, jnp.where(even, from_boxes, from_halo), 0.0)

    half_width = coupling_mine.shape[-1]
    own_half = coupling_mine[0, 0]
    their_half = coupling_other[0, 0]
    first = jnp.where(even, own_half.astype(F32), their_half.astype(F32)).astype(BF16)
    second = jnp.where(even, their_half.astype(F32), own_half.astype(F32)).astype(BF16)
    weights[:, 0:half_width] = first
    weights[:, half_width:] = second
    lane = lax.broadcasted_iota(jnp.int32, (16, s_width), 1) // rank
    wide_gap = jnp.abs(lane - here_y) > 1
    start = half + c_width + 2 * b_width
    step = jnp.where(even, 1, -1)
    sources = [
        (z, coarse[...]),
        (lax.rem(z - step + n_z, n_z), halo[:, start:]),
        (lax.rem(z + step + n_z, n_z), boxes[:, 2 * b_width :]),
    ]
    for d, part in enumerate(far_parts):
        sources.append((lax.rem(z - (d + 2) + n_z, n_z), part[...]))
    coarse_far = None
    for place, value in sources:
        far = jnp.logical_or(wide_gap, jnp.abs(place - z) > 1)
        chosen = jnp.where(far, value.astype(F32), 0.0).astype(BF16)
        columns = pl.ds(pl.multiple_of(place * s_width, s_width), s_width)
        part = nt(chosen, weights[:, columns])
        coarse_far = part if coarse_far is None else coarse_far + part
    coarse_far = split(fold(coarse_far))

    box_down = []
    for v in range(cols // 2):
        listed = jnp.where(
            even,
            pick_slots(box_window, 0, 0, v, rank),
            pick_slots(box_window, 0, 1, v, rank),
        )
        value = nt(split(listed), box_coupling[0, v]) + nt(coarse_far, box_up[0, v])
        box_down.append(split(fold(value)))

    for u in range(rows):
        for c in range(cols):
            w, v = c // 2, c % 2
            listed = split(pick_slots(leaf_window, 2 * w * rank, u, v, rank))
            down = nt(listed, leaf_coupling[u, c]) + nt(box_down[w], leaf_up[u, c])
            values = fold(nn(split(fold(down)), basis[u, c]))
            copies[u, c].wait()
            outer = nt(blocks[u, c], rim[u][:, c * n_points : (c + 3) * n_points])
            values = values + near_own[u, c] + outer.T
            chosen = one_hot(order[u, c : c + 1, :], n_points)
            out[u, c] = fold(nt(split(values), chosen))


def fetching(kernel, fetch, n_in, *refs):
    count = len(fetch)
    places, arrived = refs[len(refs) - count - 1 : -1], refs[-1]
    given = list(refs[:n_in])
    copies = {}
    for k, operand in enumerate(fetch):
        copies[operand] = pltpu.make_async_copy(refs[operand], places[k], arrived.at[k])
        copies[operand].start()
        given[operand] = places[k]
    kernel(copies, *given, *refs[n_in : len(refs) - count - 1])


def call(kernel, outs, operands, scratch=(), flops=0, limit=8, hbm=(), fetch=(), name=None):
    inside = pl.BlockSpec(memory_space=pltpu.VMEM)
    outside = pl.BlockSpec(memory_space=pltpu.HBM)
    scratch = list(scratch)
    operands = [
        pltpu.with_memory_space_constraint(value, pltpu.HBM) if k in hbm + fetch else value
        for k, value in enumerate(operands)
    ]
    if fetch:
        kernel = functools.partial(
            fetching, kernel, fetch, len(operands)
        )
        scratch += [pltpu.VMEM(operands[k].shape, operands[k].dtype) for k in fetch]
        scratch.append(pltpu.SemaphoreType.DMA((len(fetch),)))
    return pl.pallas_call(
        kernel,
        out_shape=outs,
        in_specs=[outside if k in hbm + fetch else inside for k in range(len(operands))],
        out_specs=jax.tree.map(lambda _: inside, outs),
        scratch_shapes=scratch,
        cost_estimate=pl.CostEstimate(flops=flops, bytes_accessed=0, transcendentals=0),
        compiler_params=pltpu.CompilerParams(vmem_limit_bytes=limit << 20),
        name=name,
    )(*operands)


def body(
    n_gx,
    n_gy,
    right_sides,
    leaf_order,
    leaf_basis,
    near_blocks,
    leaf_coupling,
    leaf_transfer,
    box_coupling,
    box_transfer,
    coarse_coupling,
):
    rows, cols, n_rhs, n_points = right_sides.shape
    rank = leaf_basis.shape[2]
    n_z = n_gx // 2
    tall = 2 * n_rhs
    shape = jax.ShapeDtypeStruct

    def move(value, pairs):
        return lax.ppermute(value, "gx", pairs)

    swap = [(i, i ^ 1) for i in range(n_gx)]

    def along(by):
        return [(i, 2 * ((i // 2 + by[i % 2]) % n_z) + i % 2) for i in range(n_gx)]

    coupling_other = move(coarse_coupling, swap)
    send_width = 2 * n_points + 2 * cols * rank + 4 * rank
    pts, send = call(
        up_kernel,
        (shape((tall, cols * n_points), BF16), shape((tall, send_width), BF16)),
        (right_sides, leaf_order, leaf_basis, leaf_transfer, box_transfer),
        fetch=(1, 0, 2, 3, 4),
        name="up",
    )
    gathered = lax.all_gather(send, "gy", axis=0)
    gathered, coupling_other = lax.optimization_barrier((gathered, coupling_other))
    p_width = (cols + 2) * n_points
    c_width = 2 * (cols + 4) * rank
    b_width = 6 * rank
    s_width = n_gy * rank
    mine = call(
        functools.partial(strip_kernel, n_gy, rank, n_points, cols),
        shape((tall, p_width + c_width + b_width + s_width), BF16),
        (pts, send, gathered),
        name="strip",
    )
    other = move(mine, swap)
    near_own = call(
        functools.partial(near_own_kernel, n_points),
        shape((rows, cols, n_rhs, n_points), F32),
        (mine, near_blocks),
        flops=2 * tall * 6 * rows * cols * n_points * n_points,
        limit=16,
        hbm=(1,),
        scratch=(
            pltpu.VMEM((rows, cols, n_points, 6 * n_points), BF16),
            pltpu.SemaphoreType.DMA((rows, cols)),
        ),
        name="near_own",
    )
    other, near_own = lax.optimization_barrier((other, near_own))
    halo, boxes, coarse = call(
        functools.partial(relay_kernel, n_gy, rank, n_points, cols),
        (
            shape((tall, p_width // 2 + c_width + 2 * b_width + s_width), BF16),
            shape((tall, 2 * b_width + s_width), BF16),
            shape((tall, s_width), BF16),
        ),
        (mine, other),
        name="relay",
    )
    halo_in = move(halo, along((1, -1)))
    boxes_in = move(boxes, along((-1, 1)))
    far_parts = [move(coarse, along((d, d))) for d in range(2, n_z - 1)]
    return call(
        functools.partial(down_kernel, n_gx, n_gy),
        shape((rows, cols, n_rhs, n_points), F32),
        (
            leaf_order,
            leaf_basis,
            near_blocks,
            leaf_coupling,
            leaf_transfer,
            box_coupling,
            box_transfer,
            coarse_coupling,
            coupling_other,
            mine,
            other,
            halo_in,
            boxes_in,
            coarse,
            *far_parts,
            near_own,
        ),
        scratch=(
            pltpu.VMEM((6, n_rhs, (cols + 4) * rank), F32),
            pltpu.VMEM((6, n_rhs, b_width), F32),
            pltpu.VMEM((rank, n_z * s_width), BF16),
            pltpu.VMEM((rows, cols, n_points, 3 * n_points), BF16),
            pltpu.SemaphoreType.DMA((rows, cols)),
        ),
        limit=16,
        hbm=(2,),
        name="down",
    )


def solution(mesh):
    spec = P("gx", "gy")
    return jax.shard_map(
        functools.partial(body, mesh.shape["gx"], mesh.shape["gy"]),
        mesh=mesh,
        in_specs=(spec,) * 9,
        out_specs=spec,
        check_vma=False,
    )
```

```python
import functools

import jax
import jax.numpy as jnp
from jax import lax
from jax.experimental import pallas as pl
from jax.experimental.pallas import tpu as pltpu
from jax.sharding import PartitionSpec as P

F32 = jnp.float32
BF16 = jnp.bfloat16


def nt(a, b):
    return lax.dot_general(a, b, (((1,), (1,)), ((), ())), preferred_element_type=F32)


def nn(a, b):
    return lax.dot_general(a, b, (((1,), (0,)), ((), ())), preferred_element_type=F32)


def split(x):
    hi = x.astype(BF16).astype(F32)
    return jnp.concatenate([hi, x - hi], 0).astype(BF16)


def join(y):
    half = y.shape[0] // 2
    wide = y.astype(F32)
    return wide[:half] + wide[half:]


def fold(x):
    half = x.shape[0] // 2
    return x[:half] + x[half:]


def one_hot(order_row, n_points):
    place = lax.broadcasted_iota(jnp.int32, (n_points, n_points), 0)
    return (place == order_row).astype(F32).astype(BF16)


def slot_list(u, v):
    return [
        (a, b) for a in range(6) for b in range(6) if max(abs(a - 2 - u), abs(b - 2 - v)) > 1
    ]


def pick_slots(row_of, u, v, rank, first, last):
    slots = slot_list(u, v)
    lane = None
    cache = {}

    def half(place, side):
        if place >= len(slots):
            return None
        a, b = slots[place]
        row = row_of(a)
        if row is None:
            return None
        key = (a, b // 2, b % 2 != side)
        if key not in cache:
            value = row[:, (b // 2) * 2 * rank : (b // 2 + 1) * 2 * rank]
            cache[key] = pltpu.roll(value, rank, 1) if key[2] else value
        return cache[key]

    shape = (8, 2 * rank)
    lane = lax.broadcasted_iota(jnp.int32, shape, 1)
    zero = jnp.zeros(shape, F32)
    pieces = []
    for k in range(first, last, 2):
        left, right = half(k, 0), half(k + 1, 1)
        if k + 1 == last:
            pieces.append((zero if left is None else left)[:, :rank])
        elif left is right:
            pieces.append(zero if left is None else left)
        else:
            left = zero if left is None else left
            right = zero if right is None else right
            pieces.append(jnp.where(lane < rank, left, right))
    return jnp.concatenate(pieces, 1)


def up_kernel(copies, rs, order, basis, leaf_up, box_up, pts, send):
    rows, cols, n_rhs, n_points = rs.shape
    rank = basis.shape[2]
    coeff_rows = [[] for _ in range(rows)]
    copies[1].wait()
    copies[0].wait()
    copies[2].wait()
    columns = []
    for c in range(cols):
        pair = []
        for u in range(rows):
            chosen = one_hot(order[u, c : c + 1, :], n_points)
            ordered = nn(rs[u, c], chosen)
            pair.append(ordered)
            coeff_rows[u].append(nt(ordered.astype(BF16), basis[u, c]))
        column = jnp.concatenate(pair, 0).astype(BF16)
        columns.append(column)
        pts[:, c * n_points : (c + 1) * n_points] = column
    send[:, 0:n_points] = columns[0]
    send[:, n_points : 2 * n_points] = columns[-1]
    at = 2 * n_points
    wide = [jnp.concatenate(row, 1) for row in coeff_rows]
    coeffs = [split(row) for row in wide]
    for u in range(rows):
        send[:, at : at + cols * rank] = coeffs[u]
        at += cols * rank
    boxes = []
    copies[3].wait()
    copies[4].wait()
    for w in range(cols // 2):
        total = None
        for u in range(rows):
            part = nn(
                coeffs[u][:, 2 * w * rank : 2 * (w + 1) * rank],
                leaf_up[u, 2 * w : 2 * w + 2].reshape(2 * rank, rank),
            )
            total = part if total is None else total + part
        boxes.append(fold(total))
    boxes = split(jnp.concatenate(boxes, 1))
    send[:, at : at + 2 * rank] = boxes
    at += 2 * rank
    share = fold(nn(boxes, box_up[0].reshape(2 * rank, rank)))
    send[:, at : at + 2 * rank] = split(jnp.concatenate([share, share], 1))


def masked(flag, value):
    return jnp.where(flag, value.astype(F32), 0.0).astype(BF16)


def strip_kernel(n_gy, rank, n_points, cols, pts, send, gathered, out, to_pair, to_next):
    here = lax.axis_index("gy")
    even = lax.axis_index("gx") % 2 == 0
    left = jnp.maximum(here - 1, 0)
    right = jnp.minimum(here + 1, n_gy - 1)
    has_left, has_right = here > 0, here < n_gy - 1
    first = masked(has_left, gathered[left, :, n_points : 2 * n_points])
    last = masked(has_right, gathered[right, :, 0:n_points])
    line = jnp.concatenate([first, pts[...], last], 1)
    at = (cols + 2) * n_points
    out[:, 0:at] = line
    half = at // 2
    wide = line.astype(F32)
    upper, lower = wide[:8], wide[8:]
    for row, target in (
        (jnp.where(even, lower, upper), to_pair),
        (jnp.where(even, upper, lower), to_next),
    ):
        target[:, 0:half] = jnp.concatenate([row[:, :half], row[:, half:]], 0).astype(BF16)
    source = 2 * n_points
    width = cols * rank
    pieces = []
    for u in range(2):
        pieces += [
            masked(has_left, gathered[left, :, source + width - 2 * rank : source + width]),
            send[:, source : source + width],
            masked(has_right, gathered[right, :, source : source + 2 * rank]),
        ]
        source += width
    coeffs = jnp.concatenate(pieces, 1)
    c_width = coeffs.shape[1]
    out[:, at : at + c_width] = coeffs
    to_pair[:, half : half + c_width] = coeffs
    to_next[:, half : half + c_width] = coeffs
    pieces = [
        masked(has_left, gathered[left, :, source : source + 2 * rank]),
        send[:, source : source + 2 * rank],
        masked(has_right, gathered[right, :, source : source + 2 * rank]),
    ]
    source += 2 * rank
    lane = lax.broadcasted_iota(jnp.int32, (send.shape[0], 2 * rank), 1)
    for k in range(n_gy // 2):
        low = gathered[2 * k, :, source : source + 2 * rank].astype(F32)
        high = gathered[2 * k + 1, :, source : source + 2 * rank].astype(F32)
        pieces.append(jnp.where(lane < rank, low, high).astype(BF16))
    rest = jnp.concatenate(pieces, 1)
    out[:, at + c_width :] = rest
    to_pair[:, half + c_width :] = rest


def near_own_kernel(n_points, mine, near, order, out, scatter):
    rows, cols = out.shape[0], out.shape[1]
    wide = mine[:, 0 : (cols + 2) * n_points].astype(F32)
    top, bottom = wide[:8].astype(BF16), wide[8:].astype(BF16)
    for c in range(cols):
        span = slice(c * n_points, (c + 3) * n_points)
        points = jnp.concatenate([top[:, span], bottom[:, span]], 1)
        for u in range(rows):
            first = 3 * n_points * (1 - u)
            out[u, c] = nt(near[u, c, :, first : first + 6 * n_points], points).T
    places = jnp.concatenate([order[u] for u in range(rows)], 0).astype(F32).T
    lane = lax.broadcasted_iota(jnp.int32, (n_points, n_points), 1).astype(F32)
    for u in range(rows):
        for c in range(cols):
            k = u * cols + c
            scatter[u, c] = (places[:, k : k + 1] == lane).astype(F32).astype(BF16)


def mid_kernel(
    n_gx, mine, pair, beyond, near, leaf_coupling, coupling_mine, coupling_other, near_own, near_out,
    leaf_out, weights,
):
    rows, cols, _, n_points = near_own.shape
    rank = leaf_coupling.shape[2]
    here = lax.axis_index("gx")
    even = here % 2 == 0
    has_beyond = jnp.logical_and(here > 0, here < n_gx - 1)
    p_width = (cols + 2) * n_points
    half = p_width // 2
    row_width = (cols + 4) * rank

    lines = {}
    for u in range(rows):
        lines[2 + u] = join(mine[:, p_width + u * row_width : p_width + (u + 1) * row_width])
        span = slice(half + u * row_width, half + (u + 1) * row_width)
        from_pair = join(pair[:, span])
        from_beyond = jnp.where(has_beyond, join(beyond[:, span]), 0.0)
        lines[u] = jnp.where(even, from_beyond, from_pair)
        lines[4 + u] = jnp.where(even, from_pair, from_beyond)
    for c in range(cols):
        w, v = c // 2, c % 2
        window = {a: line[:, 2 * w * rank : (2 * w + 6) * rank] for a, line in lines.items()}
        for u in range(rows):
            listed = split(pick_slots(window.get, u, v, rank, 0, 27))
            leaf_out[u, c] = fold(nt(listed, leaf_coupling[u, c]))

    from_pair = pair[:, 0:half].astype(F32)
    from_beyond = jnp.where(has_beyond, beyond[:, 0:half].astype(F32), 0.0)
    above = jnp.where(even, from_beyond, from_pair)
    below = jnp.where(even, from_pair, from_beyond)
    for u, line in enumerate((above, below)):
        points = jnp.concatenate([line[:8], line[8:]], 1).astype(BF16)
        first = 6 * u * n_points
        for c in range(cols):
            outer = nt(
                near[u, c, :, first : first + 3 * n_points],
                points[:, c * n_points : (c + 3) * n_points],
            )
            near_out[u, c] = near_own[u, c] + outer.T

    half_width = coupling_mine.shape[-1]
    own_half = coupling_mine[0, 0].astype(F32)
    their_half = coupling_other[0, 0].astype(F32)
    weights[:, 0:half_width] = jnp.where(even, own_half, their_half).astype(BF16)
    weights[:, half_width:] = jnp.where(even, their_half, own_half).astype(BF16)


def relay_kernel(b_width, mine, other, boxes, coarse):
    even = lax.axis_index("gx") % 2 == 0
    width = mine.shape[1] - boxes.shape[1] + b_width
    a_box = mine[:, width : width + b_width].astype(F32)
    total = split(join(mine[:, width + b_width :]) + join(other[:, -coarse.shape[1] :]))
    start = other.shape[1] - coarse.shape[1] - b_width
    b_box = other[:, start : start + b_width].astype(F32)
    boxes[:, 0:b_width] = jnp.where(even, a_box, b_box).astype(BF16)
    boxes[:, b_width : 2 * b_width] = jnp.where(even, b_box, a_box).astype(BF16)
    boxes[:, 2 * b_width :] = total
    coarse[...] = total


def down_kernel(
    n_gx,
    n_gy,
    basis,
    leaf_up,
    box_coupling,
    box_up,
    boxes,
    from_up,
    from_down,
    near_part,
    leaf_part,
    weights,
    scatter,
    *rest,
):
    far_parts, out = rest[:-1], rest[-1]
    rows, cols, rank, _ = basis.shape
    n_z = n_gx // 2
    here_x = lax.axis_index("gx")
    here_y = lax.axis_index("gy")
    even = here_x % 2 == 0
    z = here_x // 2
    b_width = 6 * rank
    s_width = n_gy * rank

    lane = lax.broadcasted_iota(jnp.int32, (16, s_width), 1) // rank
    wide_gap = jnp.abs(lane - here_y) > 1
    sources = [
        (z, boxes[:, 2 * b_width :]),
        (lax.rem(z - 1 + n_z, n_z), from_up[:, 2 * b_width :]),
        (lax.rem(z + 1, n_z), from_down[:, 2 * b_width :]),
    ]
    for d, part in enumerate(far_parts):
        sources.append((lax.rem(z - (d + 2) + n_z, n_z), part[...]))
    coarse_far = None
    for place, value in sources:
        far = jnp.logical_or(wide_gap, jnp.abs(place - z) > 1)
        chosen = jnp.where(far, value.astype(F32), 0.0).astype(BF16)
        columns = pl.ds(pl.multiple_of(place * s_width, s_width), s_width)
        part = nt(chosen, weights[:, columns])
        coarse_far = part if coarse_far is None else coarse_far + part
    coarse_far = split(fold(coarse_far))

    box_rows = {}
    for u in range(2):
        span = slice(u * b_width, (u + 1) * b_width)
        box_rows[u] = jnp.where(z > 0, join(from_up[:, span]), 0.0)
        box_rows[2 + u] = join(boxes[:, span])
        box_rows[4 + u] = jnp.where(z < n_z - 1, join(from_down[:, span]), 0.0)
    box_down = []
    for v in range(cols // 2):
        listed = split(
            jnp.where(
                even,
                pick_slots(box_rows.get, 0, v, rank, 0, 27),
                pick_slots(box_rows.get, 1, v, rank, 0, 27),
            )
        )
        value = nt(listed, box_coupling[0, v]) + nt(coarse_far, box_up[0, v])
        box_down.append(split(fold(value)))

    for u in range(rows):
        for c in range(cols):
            down = leaf_part[u, c] + fold(nt(box_down[c // 2], leaf_up[u, c]))
            values = fold(nn(split(down), basis[u, c])) + near_part[u, c]
            out[u, c] = fold(nn(split(values), scatter[u, c]))


def fetching(kernel, fetch, n_in, *refs):
    count = len(fetch)
    places, arrived = refs[len(refs) - count - 1 : -1], refs[-1]
    given = list(refs[:n_in])
    copies = {}
    for k, operand in enumerate(fetch):
        copies[operand] = pltpu.make_async_copy(refs[operand], places[k], arrived.at[k])
        copies[operand].start()
        given[operand] = places[k]
    kernel(copies, *given, *refs[n_in : len(refs) - count - 1])


def call(kernel, outs, operands, scratch=(), flops=0, limit=8, hbm=(), fetch=(), name=None):
    inside = pl.BlockSpec(memory_space=pltpu.VMEM)
    outside = pl.BlockSpec(memory_space=pltpu.HBM)
    scratch = list(scratch)
    operands = [
        pltpu.with_memory_space_constraint(value, pltpu.HBM) if k in hbm + fetch else value
        for k, value in enumerate(operands)
    ]
    if fetch:
        kernel = functools.partial(
            fetching, kernel, fetch, len(operands)
        )
        scratch += [pltpu.VMEM(operands[k].shape, operands[k].dtype) for k in fetch]
        scratch.append(pltpu.SemaphoreType.DMA((len(fetch),)))
    return pl.pallas_call(
        kernel,
        out_shape=outs,
        in_specs=[outside if k in hbm + fetch else inside for k in range(len(operands))],
        out_specs=jax.tree.map(lambda _: inside, outs),
        scratch_shapes=scratch,
        cost_estimate=pl.CostEstimate(flops=flops, bytes_accessed=0, transcendentals=0),
        compiler_params=pltpu.CompilerParams(vmem_limit_bytes=limit << 20),
        name=name,
    )(*operands)


def body(
    n_gx,
    n_gy,
    right_sides,
    leaf_order,
    leaf_basis,
    near_blocks,
    leaf_coupling,
    leaf_transfer,
    box_coupling,
    box_transfer,
    coarse_coupling,
):
    rows, cols, n_rhs, n_points = right_sides.shape
    rank = leaf_basis.shape[2]
    n_z = n_gx // 2
    tall = 2 * n_rhs
    shape = jax.ShapeDtypeStruct

    def move(value, pairs):
        return lax.ppermute(value, "gx", pairs)

    swap = [(i, i ^ 1) for i in range(n_gx)]

    def along(by):
        return [(i, 2 * ((i // 2 + by) % n_z) + i % 2) for i in range(n_gx)]

    last = n_gx - 1
    outward = [(i, i if i in (0, last) else i - 1 + 2 * (i % 2)) for i in range(n_gx)]

    coupling_other = move(coarse_coupling, swap)
    send_width = 2 * n_points + 2 * cols * rank + 4 * rank
    pts, send = call(
        up_kernel,
        (shape((tall, cols * n_points), BF16), shape((tall, send_width), BF16)),
        (right_sides, leaf_order, leaf_basis, leaf_transfer, box_transfer),
        fetch=(1, 0, 2, 3, 4),
        flops=50000000000,
        name="up",
    )
    gathered = lax.all_gather(send, "gy", axis=0)
    gathered, coupling_other = lax.optimization_barrier((gathered, coupling_other))
    p_width = (cols + 2) * n_points
    c_width = 2 * (cols + 4) * rank
    b_width = 6 * rank
    s_width = n_gy * rank
    rest_width = p_width // 2 + c_width
    mine, to_pair, to_next = call(
        functools.partial(strip_kernel, n_gy, rank, n_points, cols),
        (
            shape((tall, p_width + c_width + b_width + s_width), BF16),
            shape((tall, rest_width + b_width + s_width), BF16),
            shape((tall, rest_width), BF16),
        ),
        (pts, send, gathered),
        flops=50000000000,
        name="strip",
    )
    pair = move(to_pair, swap)
    near_own, scatter = call(
        functools.partial(near_own_kernel, n_points),
        (
            shape((rows, cols, n_rhs, n_points), F32),
            shape((rows, cols, n_points, n_points), BF16),
        ),
        (mine, near_blocks, leaf_order),
        flops=2 * tall * 6 * rows * cols * n_points * n_points,
        limit=8,
        name="near_own",
    )
    pair, near_own = lax.optimization_barrier((pair, near_own))
    boxes, coarse = call(
        functools.partial(relay_kernel, b_width),
        (shape((tall, 2 * b_width + s_width), BF16), shape((tall, s_width), BF16)),
        (mine, pair),
        name="relay",
    )
    to_next, boxes, coarse = lax.optimization_barrier((to_next, boxes, coarse))
    beyond = move(to_next, outward)
    from_up = move(boxes, along(1))
    from_down = move(boxes, along(-1))
    far_parts = [move(coarse, along(d)) for d in range(2, n_z - 1)]
    near_part, leaf_part, weights = call(
        functools.partial(mid_kernel, n_gx),
        (
            shape((rows, cols, n_rhs, n_points), F32),
            shape((rows, cols, n_rhs, rank), F32),
            shape((rank, n_z * s_width), BF16),
        ),
        (
            mine,
            pair,
            beyond,
            near_blocks,
            leaf_coupling,
            coarse_coupling,
            coupling_other,
            near_own,
        ),
        flops=1000000000,
        limit=8,
        name="mid",
    )
    return call(
        functools.partial(down_kernel, n_gx, n_gy),
        shape((rows, cols, n_rhs, n_points), F32),
        (
            leaf_basis,
            leaf_transfer,
            box_coupling,
            box_transfer,
            boxes,
            from_up,
            from_down,
            near_part,
            leaf_part,
            weights,
            scatter,
            *far_parts,
        ),
        limit=8,
        name="down",
    )


def solution(mesh):
    spec = P("gx", "gy")
    return jax.shard_map(
        functools.partial(body, mesh.shape["gx"], mesh.shape["gy"]),
        mesh=mesh,
        in_specs=(spec,) * 9,
        out_specs=spec,
        check_vma=False,
    )
```

```python
import functools

import jax
import jax.numpy as jnp
from jax import lax
from jax.experimental import pallas as pl
from jax.experimental.pallas import tpu as pltpu
from jax.sharding import PartitionSpec as P


F32 = jnp.float32
BF16 = jnp.bfloat16


def nt(a, b):
    return lax.dot_general(a, b, (((1,), (1,)), ((), ())), preferred_element_type=F32)


def nn(a, b):
    return lax.dot_general(a, b, (((1,), (0,)), ((), ())), preferred_element_type=F32)


def split(x):
    hi = x.astype(BF16).astype(F32)
    return jnp.concatenate([hi, x - hi], 0).astype(BF16)


def join(y):
    half = y.shape[0] // 2
    wide = y.astype(F32)
    return wide[:half] + wide[half:]


def fold(x):
    half = x.shape[0] // 2
    return x[:half] + x[half:]


def one_hot(order_row, n_points):
    place = lax.broadcasted_iota(jnp.int32, (n_points, n_points), 0)
    return (place == order_row).astype(F32).astype(BF16)


def slot_list(u, v):
    return [
        (a, b) for a in range(6) for b in range(6) if max(abs(a - 2 - u), abs(b - 2 - v)) > 1
    ]


def pick_slots(row_of, u, v, rank, first, last):
    slots = slot_list(u, v)
    lane = None
    cache = {}

    def half(place, side):
        if place >= len(slots):
            return None
        a, b = slots[place]
        row = row_of(a)
        if row is None:
            return None
        key = (a, b // 2, b % 2 != side)
        if key not in cache:
            value = row[:, (b // 2) * 2 * rank : (b // 2 + 1) * 2 * rank]
            cache[key] = pltpu.roll(value, rank, 1) if key[2] else value
        return cache[key]

    shape = (8, 2 * rank)
    lane = lax.broadcasted_iota(jnp.int32, shape, 1)
    zero = jnp.zeros(shape, F32)
    pieces = []
    for k in range(first, last, 2):
        left, right = half(k, 0), half(k + 1, 1)
        if k + 1 == last:
            pieces.append((zero if left is None else left)[:, :rank])
        elif left is right:
            pieces.append(zero if left is None else left)
        else:
            left = zero if left is None else left
            right = zero if right is None else right
            pieces.append(jnp.where(lane < rank, left, right))
    return jnp.concatenate(pieces, 1)


def pick_by_parity(even, even_rows, odd_rows, u, v, rank, even_span, odd_span):
    return split(
        jnp.where(
            even,
            pick_slots(even_rows.get, u, v, rank, *even_span),
            pick_slots(odd_rows.get, u, v, rank, *odd_span),
        )
    )


def up_kernel(copies, rs, order, basis, leaf_up, box_up, pts, send):
    rows, cols, _, n_points = rs.shape
    rank = basis.shape[2]
    coeff_rows = [[] for _ in range(rows)]
    copies[1].wait()
    copies[0].wait()
    copies[2].wait()
    columns = []
    for c in range(cols):
        pair = []
        for u in range(rows):
            chosen = one_hot(order[u, c : c + 1, :], n_points)
            ordered = nn(rs[u, c], chosen)
            pair.append(ordered)
            coeff_rows[u].append(nt(ordered.astype(BF16), basis[u, c]))
        column = jnp.concatenate(pair, 0).astype(BF16)
        columns.append(column)
        pts[:, c * n_points : (c + 1) * n_points] = column
    send[:, 0:n_points] = columns[0]
    send[:, n_points : 2 * n_points] = columns[-1]
    at = 2 * n_points
    wide = [jnp.concatenate(row, 1) for row in coeff_rows]
    coeffs = [split(row) for row in wide]
    for u in range(rows):
        send[:, at : at + cols * rank] = coeffs[u]
        at += cols * rank
    boxes = []
    copies[3].wait()
    copies[4].wait()
    for w in range(cols // 2):
        total = None
        for u in range(rows):
            part = nn(
                coeffs[u][:, 2 * w * rank : 2 * (w + 1) * rank],
                leaf_up[u, 2 * w : 2 * w + 2].reshape(2 * rank, rank),
            )
            total = part if total is None else total + part
        boxes.append(fold(total))
    boxes = split(jnp.concatenate(boxes, 1))
    send[:, at : at + 2 * rank] = boxes
    at += 2 * rank
    share = fold(nn(boxes, box_up[0].reshape(2 * rank, rank)))
    send[:, at : at + 2 * rank] = split(jnp.concatenate([share, share], 1))


def masked(flag, value):
    return jnp.where(flag, value.astype(F32), 0.0).astype(BF16)


def strip_kernel(n_gy, rank, n_points, cols, pts, send, gathered, out):
    here = lax.axis_index("gy")
    left = jnp.maximum(here - 1, 0)
    right = jnp.minimum(here + 1, n_gy - 1)
    has_left, has_right = here > 0, here < n_gy - 1
    out[:, 0:n_points] = masked(has_left, gathered[left, :, n_points : 2 * n_points])
    out[:, n_points : (cols + 1) * n_points] = pts[...]
    at = (cols + 2) * n_points
    out[:, at - n_points : at] = masked(has_right, gathered[right, :, 0:n_points])
    source = 2 * n_points
    width = cols * rank
    for _ in range(2):
        out[:, at : at + 2 * rank] = masked(
            has_left, gathered[left, :, source + width - 2 * rank : source + width]
        )
        at += 2 * rank
        out[:, at : at + width] = send[:, source : source + width]
        at += width
        out[:, at : at + 2 * rank] = masked(
            has_right, gathered[right, :, source : source + 2 * rank]
        )
        at += 2 * rank
        source += width
    out[:, at : at + 2 * rank] = masked(has_left, gathered[left, :, source : source + 2 * rank])
    out[:, at + 2 * rank : at + 4 * rank] = send[:, source : source + 2 * rank]
    out[:, at + 4 * rank : at + 6 * rank] = masked(
        has_right, gathered[right, :, source : source + 2 * rank]
    )
    at += 6 * rank
    source += 2 * rank
    lane = lax.broadcasted_iota(jnp.int32, (send.shape[0], 2 * rank), 1)
    for k in range(n_gy // 2):
        low = gathered[2 * k, :, source : source + 2 * rank].astype(F32)
        high = gathered[2 * k + 1, :, source : source + 2 * rank].astype(F32)
        out[:, at : at + 2 * rank] = jnp.where(lane < rank, low, high).astype(BF16)
        at += 2 * rank


def near_own_kernel(n_points, mine, near, order, out, scatter):
    rows, cols = out.shape[0], out.shape[1]
    wide = mine[:, 0 : (cols + 2) * n_points].astype(F32)
    top, bottom = wide[:8].astype(BF16), wide[8:].astype(BF16)
    for c in range(cols):
        span = slice(c * n_points, (c + 3) * n_points)
        points = jnp.concatenate([top[:, span], bottom[:, span]], 1)
        for u in range(rows):
            first = 3 * n_points * (1 - u)
            out[u, c] = nt(near[u, c, :, first : first + 6 * n_points], points).T
    places = jnp.concatenate([order[u] for u in range(rows)], 0).astype(F32).T
    lane = lax.broadcasted_iota(jnp.int32, (n_points, n_points), 1).astype(F32)
    for u in range(rows):
        for c in range(cols):
            k = u * cols + c
            scatter[u, c] = (places[:, k : k + 1] == lane).astype(F32).astype(BF16)


def mid_kernel(
    mine, other, near, leaf_coupling, coupling_mine, coupling_other, near_own, near_out, leaf_out,
    weights,
):
    rows, cols, _, n_points = near_own.shape
    rank = leaf_coupling.shape[2]
    parity = lax.axis_index("gx") % 2
    even = parity == 0
    p_width = (cols + 2) * n_points
    row_width = (cols + 4) * rank

    wide = other[:, 0:p_width].astype(F32)
    rim = jnp.where(even, wide[:8], wide[8:]).astype(BF16)
    touched = 1 - parity
    columns = pl.ds(pl.multiple_of(touched * 6 * n_points, 6 * n_points), 3 * n_points)
    for c in range(cols):
        points = rim[:, c * n_points : (c + 3) * n_points]
        outer = nt(near[touched, c, :, columns], points).T
        near_out[touched, c] = near_own[touched, c] + outer
        near_out[parity, c] = near_own[parity, c]

    own, theirs = [], []
    for u in range(rows):
        span = slice(p_width + u * row_width, p_width + (u + 1) * row_width)
        own.append(join(mine[:, span]))
        theirs.append(join(other[:, span]))
    start = pl.multiple_of(jnp.where(even, 8 * rank, 0), 2 * rank)
    for c in range(cols):
        w, v = c // 2, c % 2
        window = slice(2 * w * rank, (2 * w + 6) * rank)
        mine_rows = {2: own[0][:, window], 3: own[1][:, window]}
        even_rows = {**mine_rows, 4: theirs[0][:, window], 5: theirs[1][:, window]}
        odd_rows = {**mine_rows, 0: theirs[0][:, window], 1: theirs[1][:, window]}
        for u in range(rows):
            listed = pick_by_parity(even, even_rows, odd_rows, u, v, rank, (8, 27), (0, 19))
            leaf_out[u, c] = fold(nt(listed, leaf_coupling[u, c, :, pl.ds(start, 19 * rank)]))

    half_width = coupling_mine.shape[-1]
    own_half = coupling_mine[0, 0].astype(F32)
    their_half = coupling_other[0, 0].astype(F32)
    weights[:, 0:half_width] = jnp.where(even, own_half, their_half).astype(BF16)
    weights[:, half_width:] = jnp.where(even, their_half, own_half).astype(BF16)


def relay_kernel(rank, n_points, cols, mine, other, halo, boxes, coarse):
    parity = lax.axis_index("gx") % 2
    even = parity == 0
    p_width = (cols + 2) * n_points
    c_width = 2 * (cols + 4) * rank
    b_width = 6 * rank
    wide = other[:, 0:p_width].astype(F32)
    row = jnp.where(even, wide[8:], wide[:8])
    half = p_width // 2
    halo[:, 0:half] = jnp.concatenate([row[:, :half], row[:, half:]], 0).astype(BF16)
    halo[:, half : half + c_width] = other[:, p_width : p_width + c_width]
    at = p_width + c_width
    a_box = mine[:, at : at + b_width].astype(F32)
    b_box = other[:, at : at + b_width].astype(F32)
    top = jnp.where(even, a_box, b_box).astype(BF16)
    bottom = jnp.where(even, b_box, a_box).astype(BF16)
    total = split(join(mine[:, at + b_width :]) + join(other[:, at + b_width :]))
    to = half + c_width
    halo[:, to : to + b_width] = top
    halo[:, to + b_width : to + 2 * b_width] = bottom
    halo[:, to + 2 * b_width :] = total
    boxes[:, 0:b_width] = top
    boxes[:, b_width : 2 * b_width] = bottom
    boxes[:, 2 * b_width :] = total
    coarse[...] = total


def beyond_kernel(n_gx, halo, near, leaf_coupling, near_part, leaf_part, near_out, leaf_out):
    rows, cols, _, n_points = near_part.shape
    rank = leaf_coupling.shape[2]
    here = lax.axis_index("gx")
    parity = here % 2
    even = parity == 0
    has_halo = jnp.logical_and(here > 0, here < n_gx - 1)
    half = (cols + 2) * n_points // 2
    row_width = (cols + 4) * rank
    from_halo = []
    for u in range(rows):
        span = slice(half + u * row_width, half + (u + 1) * row_width)
        from_halo.append(jnp.where(has_halo, join(halo[:, span]), 0.0))
    start = pl.multiple_of(jnp.where(even, 0, 14 * rank), 2 * rank)
    for c in range(cols):
        w, v = c // 2, c % 2
        window = slice(2 * w * rank, (2 * w + 6) * rank)
        even_rows = {0: from_halo[0][:, window], 1: from_halo[1][:, window]}
        odd_rows = {4: from_halo[0][:, window], 5: from_halo[1][:, window]}
        for u in range(rows):
            listed = pick_by_parity(even, even_rows, odd_rows, u, v, rank, (0, 13), (14, 27))
            extra = fold(nt(listed, leaf_coupling[u, c, :, pl.ds(start, 13 * rank)]))
            leaf_out[u, c] = leaf_part[u, c] + extra
    strip = jnp.where(has_halo, halo[:, 0:half].astype(F32), 0.0)
    strip = jnp.concatenate([strip[:8], strip[8:]], 1).astype(BF16)
    columns = pl.ds(pl.multiple_of(parity * 6 * n_points, 6 * n_points), 3 * n_points)
    for c in range(cols):
        outer = nt(near[parity, c, :, columns], strip[:, c * n_points : (c + 3) * n_points]).T
        near_out[parity, c] = near_part[parity, c] + outer
        near_out[1 - parity, c] = near_part[1 - parity, c]


def down_kernel(
    n_gx,
    n_gy,
    basis,
    leaf_up,
    box_coupling,
    box_up,
    mine,
    other,
    halo,
    boxes,
    coarse,
    near_part,
    leaf_part,
    weights,
    scatter,
    *rest,
):
    far_parts, out = rest[:-1], rest[-1]
    rows, cols, rank, n_points = basis.shape
    n_z = n_gx // 2
    here_x = lax.axis_index("gx")
    here_y = lax.axis_index("gy")
    parity = here_x % 2
    even = parity == 0
    z = here_x // 2
    has_up, has_down = z > 0, z < n_z - 1
    p_width = (cols + 2) * n_points
    half = p_width // 2
    row_width = (cols + 4) * rank
    c_width = 2 * row_width
    b_width = 6 * rank
    s_width = n_gy * rank

    lane = lax.broadcasted_iota(jnp.int32, (16, s_width), 1) // rank
    wide_gap = jnp.abs(lane - here_y) > 1
    start = half + c_width + 2 * b_width
    step = jnp.where(even, 1, -1)
    sources = [
        (z, coarse[...]),
        (lax.rem(z - step + n_z, n_z), halo[:, start:]),
        (lax.rem(z + step + n_z, n_z), boxes[:, 2 * b_width :]),
    ]
    for d, part in enumerate(far_parts):
        sources.append((lax.rem(z - (d + 2) + n_z, n_z), part[...]))
    coarse_far = None
    for place, value in sources:
        far = jnp.logical_or(wide_gap, jnp.abs(place - z) > 1)
        chosen = jnp.where(far, value.astype(F32), 0.0).astype(BF16)
        columns = pl.ds(pl.multiple_of(place * s_width, s_width), s_width)
        part = nt(chosen, weights[:, columns])
        coarse_far = part if coarse_far is None else coarse_far + part
    coarse_far = split(fold(coarse_far))

    at = p_width + c_width
    a_box, b_box = join(mine[:, at : at + b_width]), join(other[:, at : at + b_width])
    box_rows = {2: jnp.where(even, a_box, b_box), 3: jnp.where(even, b_box, a_box)}
    for u in range(2):
        start = half + c_width + u * b_width
        from_halo = join(halo[:, start : start + b_width])
        from_boxes = join(boxes[:, u * b_width : (u + 1) * b_width])
        box_rows[u] = jnp.where(has_up, jnp.where(even, from_halo, from_boxes), 0.0)
        box_rows[4 + u] = jnp.where(has_down, jnp.where(even, from_boxes, from_halo), 0.0)
    box_down = []
    for v in range(cols // 2):
        listed = split(
            jnp.where(
                even,
                pick_slots(box_rows.get, 0, v, rank, 0, 27),
                pick_slots(box_rows.get, 1, v, rank, 0, 27),
            )
        )
        value = nt(listed, box_coupling[0, v]) + nt(coarse_far, box_up[0, v])
        box_down.append(split(fold(value)))

    for u in range(rows):
        for c in range(cols):
            down = leaf_part[u, c] + fold(nt(box_down[c // 2], leaf_up[u, c]))
            values = fold(nn(split(down), basis[u, c])) + near_part[u, c]
            out[u, c] = fold(nn(split(values), scatter[u, c]))


def fetching(kernel, fetch, n_in, *refs):
    count = len(fetch)
    places, arrived = refs[len(refs) - count - 1 : -1], refs[-1]
    given = list(refs[:n_in])
    copies = {}
    for k, operand in enumerate(fetch):
        copies[operand] = pltpu.make_async_copy(refs[operand], places[k], arrived.at[k])
        copies[operand].start()
        given[operand] = places[k]
    kernel(copies, *given, *refs[n_in : len(refs) - count - 1])


def call(kernel, outs, operands, scratch=(), flops=0, limit=8, hbm=(), fetch=()):
    inside = pl.BlockSpec(memory_space=pltpu.VMEM)
    outside = pl.BlockSpec(memory_space=pltpu.HBM)
    scratch = list(scratch)
    operands = [
        pltpu.with_memory_space_constraint(value, pltpu.HBM) if k in hbm + fetch else value
        for k, value in enumerate(operands)
    ]
    if fetch:
        kernel = functools.partial(
            fetching, kernel, fetch, len(operands)
        )
        scratch += [pltpu.VMEM(operands[k].shape, operands[k].dtype) for k in fetch]
        scratch.append(pltpu.SemaphoreType.DMA((len(fetch),)))
    return pl.pallas_call(
        kernel,
        out_shape=outs,
        in_specs=[outside if k in hbm + fetch else inside for k in range(len(operands))],
        out_specs=jax.tree.map(lambda _: inside, outs),
        scratch_shapes=scratch,
        cost_estimate=pl.CostEstimate(flops=flops, bytes_accessed=0, transcendentals=0),
        compiler_params=pltpu.CompilerParams(vmem_limit_bytes=limit << 20),
    )(*operands)


def body(
    n_gx,
    n_gy,
    right_sides,
    leaf_order,
    leaf_basis,
    near_blocks,
    leaf_coupling,
    leaf_transfer,
    box_coupling,
    box_transfer,
    coarse_coupling,
):
    rows, cols, n_rhs, n_points = right_sides.shape
    rank = leaf_basis.shape[2]
    n_z = n_gx // 2
    tall = 2 * n_rhs
    shape = jax.ShapeDtypeStruct

    def move(value, pairs):
        return lax.ppermute(value, "gx", pairs)

    swap = [(i, i ^ 1) for i in range(n_gx)]

    def along(by):
        return [(i, 2 * ((i // 2 + by[i % 2]) % n_z) + i % 2) for i in range(n_gx)]

    coupling_other = move(coarse_coupling, swap)
    send_width = 2 * n_points + 2 * cols * rank + 4 * rank
    pts, send = call(
        up_kernel,
        (shape((tall, cols * n_points), BF16), shape((tall, send_width), BF16)),
        (right_sides, leaf_order, leaf_basis, leaf_transfer, box_transfer),
        fetch=(1, 0, 2, 3, 4),
        flops=50000000000,
    )
    gathered = lax.all_gather(send, "gy", axis=0)
    gathered, coupling_other = lax.optimization_barrier((gathered, coupling_other))
    p_width = (cols + 2) * n_points
    c_width = 2 * (cols + 4) * rank
    b_width = 6 * rank
    s_width = n_gy * rank
    mine = call(
        functools.partial(strip_kernel, n_gy, rank, n_points, cols),
        shape((tall, p_width + c_width + b_width + s_width), BF16),
        (pts, send, gathered),
        flops=50000000000,
    )
    other = move(mine, swap)
    near_own, scatter = call(
        functools.partial(near_own_kernel, n_points),
        (
            shape((rows, cols, n_rhs, n_points), F32),
            shape((rows, cols, n_points, n_points), BF16),
        ),
        (mine, near_blocks, leaf_order),
        flops=2 * tall * 6 * rows * cols * n_points * n_points,
        limit=8,
    )
    other, near_own = lax.optimization_barrier((other, near_own))
    halo, boxes, coarse = call(
        functools.partial(relay_kernel, rank, n_points, cols),
        (
            shape((tall, p_width // 2 + c_width + 2 * b_width + s_width), BF16),
            shape((tall, 2 * b_width + s_width), BF16),
            shape((tall, s_width), BF16),
        ),
        (mine, other),
    )
    halo_in = move(halo, along((1, -1)))
    boxes_in = move(boxes, along((-1, 1)))
    far_parts = []
    for d in range(2, n_z - 1):
        far_parts.append(move(coarse, along((d, d))))
    near_part, leaf_part, weights = call(
        mid_kernel,
        (
            shape((rows, cols, n_rhs, n_points), F32),
            shape((rows, cols, n_rhs, rank), F32),
            shape((rank, n_z * s_width), BF16),
        ),
        (
            mine,
            other,
            near_blocks,
            leaf_coupling,
            coarse_coupling,
            coupling_other,
            near_own,
        ),
        flops=1000000000,
        limit=8,
    )
    near_part, leaf_part = call(
        functools.partial(beyond_kernel, n_gx),
        (
            shape((rows, cols, n_rhs, n_points), F32),
            shape((rows, cols, n_rhs, rank), F32),
        ),
        (halo_in, near_blocks, leaf_coupling, near_part, leaf_part),
        flops=1000000000,
        limit=8,
    )
    return call(
        functools.partial(down_kernel, n_gx, n_gy),
        shape((rows, cols, n_rhs, n_points), F32),
        (
            leaf_basis,
            leaf_transfer,
            box_coupling,
            box_transfer,
            mine,
            other,
            halo_in,
            boxes_in,
            coarse,
            near_part,
            leaf_part,
            weights,
            scatter,
            *far_parts,
        ),
        limit=8,
    )


def solution(mesh):
    spec = P("gx", "gy")
    return jax.shard_map(
        functools.partial(body, mesh.shape["gx"], mesh.shape["gy"]),
        mesh=mesh,
        in_specs=(spec,) * 9,
        out_specs=spec,
        check_vma=False,
    )
```

```python
import functools

import jax
import jax.numpy as jnp
from jax import lax
from jax.experimental import pallas as pl
from jax.experimental.pallas import tpu as pltpu
from jax.sharding import PartitionSpec as P


F32 = jnp.float32
BF16 = jnp.bfloat16


def nt(a, b):
    return lax.dot_general(a, b, (((1,), (1,)), ((), ())), preferred_element_type=F32)


def nn(a, b):
    return lax.dot_general(a, b, (((1,), (0,)), ((), ())), preferred_element_type=F32)


def split(x):
    hi = x.astype(BF16).astype(F32)
    return jnp.concatenate([hi, x - hi], 0).astype(BF16)


def join(y):
    half = y.shape[0] // 2
    wide = y.astype(F32)
    return wide[:half] + wide[half:]


def fold(x):
    half = x.shape[0] // 2
    return x[:half] + x[half:]


def one_hot(order_row, n_points):
    place = lax.broadcasted_iota(jnp.int32, (n_points, n_points), 0)
    return (place == order_row).astype(F32).astype(BF16)


def slot_list(u, v):
    return [
        (a, b) for a in range(6) for b in range(6) if max(abs(a - 2 - u), abs(b - 2 - v)) > 1
    ]


def pick_slots(row_of, u, v, rank, first, last):
    slots = slot_list(u, v)
    lane = None
    cache = {}

    def half(place, side):
        if place >= len(slots):
            return None
        a, b = slots[place]
        row = row_of(a)
        if row is None:
            return None
        key = (a, b // 2, b % 2 != side)
        if key not in cache:
            value = row[:, (b // 2) * 2 * rank : (b // 2 + 1) * 2 * rank]
            cache[key] = pltpu.roll(value, rank, 1) if key[2] else value
        return cache[key]

    shape = (8, 2 * rank)
    lane = lax.broadcasted_iota(jnp.int32, shape, 1)
    zero = jnp.zeros(shape, F32)
    pieces = []
    for k in range(first, last, 2):
        left, right = half(k, 0), half(k + 1, 1)
        if k + 1 == last:
            pieces.append((zero if left is None else left)[:, :rank])
        elif left is right:
            pieces.append(zero if left is None else left)
        else:
            left = zero if left is None else left
            right = zero if right is None else right
            pieces.append(jnp.where(lane < rank, left, right))
    return jnp.concatenate(pieces, 1)


def pick_by_parity(even, even_rows, odd_rows, u, v, rank, even_span, odd_span):
    return split(
        jnp.where(
            even,
            pick_slots(even_rows.get, u, v, rank, *even_span),
            pick_slots(odd_rows.get, u, v, rank, *odd_span),
        )
    )


def up_kernel(copies, rs, order, basis, leaf_up, box_up, pts, send):
    rows, cols, _, n_points = rs.shape
    rank = basis.shape[2]
    copies[1].wait()
    copies[0].wait()
    ordered = {}
    for c in range(cols):
        for u in range(rows):
            ordered[u, c] = nn(rs[u, c], one_hot(order[u, c : c + 1, :], n_points))
    copies[2].wait()
    coeff_rows = [
        [nt(ordered[u, c].astype(BF16), basis[u, c]) for c in range(cols)] for u in range(rows)
    ]
    columns = []
    for c in range(cols):
        column = jnp.concatenate([ordered[u, c] for u in range(rows)], 0).astype(BF16)
        columns.append(column)
        pts[:, c * n_points : (c + 1) * n_points] = column
    send[:, 0:n_points] = columns[0]
    send[:, n_points : 2 * n_points] = columns[-1]
    at = 2 * n_points
    wide = [jnp.concatenate(row, 1) for row in coeff_rows]
    coeffs = [split(row) for row in wide]
    for u in range(rows):
        send[:, at : at + cols * rank] = coeffs[u]
        at += cols * rank
    boxes = []
    copies[3].wait()
    copies[4].wait()
    for w in range(cols // 2):
        total = None
        for u in range(rows):
            part = nn(
                coeffs[u][:, 2 * w * rank : 2 * (w + 1) * rank],
                leaf_up[u, 2 * w : 2 * w + 2].reshape(2 * rank, rank),
            )
            total = part if total is None else total + part
        boxes.append(fold(total))
    boxes = split(jnp.concatenate(boxes, 1))
    send[:, at : at + 2 * rank] = boxes
    at += 2 * rank
    share = fold(nn(boxes, box_up[0].reshape(2 * rank, rank)))
    send[:, at : at + 2 * rank] = split(jnp.concatenate([share, share], 1))


def masked(flag, value):
    return jnp.where(flag, value.astype(F32), 0.0).astype(BF16)


def strip_kernel(n_gy, rank, n_points, cols, pts, send, gathered, out):
    here = lax.axis_index("gy")
    left = jnp.maximum(here - 1, 0)
    right = jnp.minimum(here + 1, n_gy - 1)
    has_left, has_right = here > 0, here < n_gy - 1
    out[:, 0:n_points] = masked(has_left, gathered[left, :, n_points : 2 * n_points])
    out[:, n_points : (cols + 1) * n_points] = pts[...]
    at = (cols + 2) * n_points
    out[:, at - n_points : at] = masked(has_right, gathered[right, :, 0:n_points])
    source = 2 * n_points
    width = cols * rank
    for _ in range(2):
        out[:, at : at + 2 * rank] = masked(
            has_left, gathered[left, :, source + width - 2 * rank : source + width]
        )
        at += 2 * rank
        out[:, at : at + width] = send[:, source : source + width]
        at += width
        out[:, at : at + 2 * rank] = masked(
            has_right, gathered[right, :, source : source + 2 * rank]
        )
        at += 2 * rank
        source += width
    out[:, at : at + 2 * rank] = masked(has_left, gathered[left, :, source : source + 2 * rank])
    out[:, at + 2 * rank : at + 4 * rank] = send[:, source : source + 2 * rank]
    out[:, at + 4 * rank : at + 6 * rank] = masked(
        has_right, gathered[right, :, source : source + 2 * rank]
    )
    at += 6 * rank
    source += 2 * rank
    lane = lax.broadcasted_iota(jnp.int32, (send.shape[0], 2 * rank), 1)
    for k in range(n_gy // 2):
        low = gathered[2 * k, :, source : source + 2 * rank].astype(F32)
        high = gathered[2 * k + 1, :, source : source + 2 * rank].astype(F32)
        out[:, at : at + 2 * rank] = jnp.where(lane < rank, low, high).astype(BF16)
        at += 2 * rank


def near_own_kernel(
    n_points, mine, near, order, basis, leaf_up, out, scatter, leaf_base, box_base
):
    rows, cols = out.shape[0], out.shape[1]
    places = jnp.concatenate([order[u] for u in range(rows)], 0).astype(F32).T
    lane = lax.broadcasted_iota(jnp.int32, (n_points, n_points), 1).astype(F32)
    wide = mine[:, 0 : (cols + 2) * n_points].astype(F32)
    top, bottom = wide[:8].astype(BF16), wide[8:].astype(BF16)
    values = {}
    for c in range(cols):
        span = slice(c * n_points, (c + 3) * n_points)
        points = jnp.concatenate([top[:, span], bottom[:, span]], 1)
        for u in range(rows):
            first = 3 * n_points * (1 - u)
            values[u, c] = nt(near[u, c, :, first : first + 6 * n_points], points)
    chosen = {}
    for c in range(cols):
        for u in range(rows):
            k = u * cols + c
            chosen[u, c] = (places[:, k : k + 1] == lane).astype(F32).astype(BF16)
            scatter[u, c] = chosen[u, c]
    moved = {}
    for u, c in chosen:
        stacked = jnp.concatenate([split(values[u, c].T), basis[u, c]], 0)
        moved[u, c] = nn(stacked, scatter[u, c])
    for u, c in chosen:
        out[u, c] = fold(moved[u, c][:16])
        moved[u, c] = moved[u, c][16:].astype(BF16)
        leaf_base[u, c] = moved[u, c]
    for u, c in chosen:
        product = nn(leaf_up[u, c].astype(F32).T.astype(BF16), moved[u, c])
        high = product.astype(BF16)
        box_base[u, c, :, 0:n_points] = high
        box_base[u, c, :, n_points:] = (product - high.astype(F32)).astype(BF16)


def mid_kernel(
    mine, other, near, leaf_coupling, coupling_mine, coupling_other, near_own, scatter, near_out,
    leaf_out, weights,
):
    rows, cols, _, n_points = near_own.shape
    rank = leaf_coupling.shape[2]
    parity = lax.axis_index("gx") % 2
    even = parity == 0
    p_width = (cols + 2) * n_points
    row_width = (cols + 4) * rank

    wide = other[:, 0:p_width].astype(F32)
    rim = jnp.where(even, wide[:8], wide[8:]).astype(BF16)
    touched = 1 - parity
    outers = []
    columns = pl.ds(pl.multiple_of(touched * 6 * n_points, 6 * n_points), 3 * n_points)
    for c in range(cols):
        points = rim[:, c * n_points : (c + 3) * n_points]
        outer = nt(near[touched, c, :, columns], points).T
        outers.append(split(outer))
        near_out[parity, c] = near_own[parity, c]

    own, theirs = [], []
    for u in range(rows):
        span = slice(p_width + u * row_width, p_width + (u + 1) * row_width)
        own.append(join(mine[:, span]))
        theirs.append(join(other[:, span]))
    start = pl.multiple_of(jnp.where(even, 8 * rank, 0), 2 * rank)
    for c in range(cols):
        w, v = c // 2, c % 2
        window = slice(2 * w * rank, (2 * w + 6) * rank)
        mine_rows = {2: own[0][:, window], 3: own[1][:, window]}
        even_rows = {**mine_rows, 4: theirs[0][:, window], 5: theirs[1][:, window]}
        odd_rows = {**mine_rows, 0: theirs[0][:, window], 1: theirs[1][:, window]}
        for u in range(rows):
            listed = pick_by_parity(even, even_rows, odd_rows, u, v, rank, (8, 27), (0, 19))
            leaf_out[u, c] = fold(nt(listed, leaf_coupling[u, c, :, pl.ds(start, 19 * rank)]))

    for c in range(cols):
        outer = fold(nn(outers[c], scatter[touched, c]))
        near_out[touched, c] = near_own[touched, c] + outer
    half_width = coupling_mine.shape[-1]
    own_half = coupling_mine[0, 0].astype(F32)
    their_half = coupling_other[0, 0].astype(F32)
    weights[:, 0:half_width] = jnp.where(even, own_half, their_half).astype(BF16)
    weights[:, half_width:] = jnp.where(even, their_half, own_half).astype(BF16)


def relay_kernel(rank, n_points, cols, mine, other, halo, boxes, coarse):
    parity = lax.axis_index("gx") % 2
    even = parity == 0
    p_width = (cols + 2) * n_points
    c_width = 2 * (cols + 4) * rank
    b_width = 6 * rank
    wide = other[:, 0:p_width].astype(F32)
    row = jnp.where(even, wide[8:], wide[:8])
    half = p_width // 2
    halo[:, 0:half] = jnp.concatenate([row[:, :half], row[:, half:]], 0).astype(BF16)
    halo[:, half : half + c_width] = other[:, p_width : p_width + c_width]
    at = p_width + c_width
    a_box = mine[:, at : at + b_width].astype(F32)
    b_box = other[:, at : at + b_width].astype(F32)
    top = jnp.where(even, a_box, b_box).astype(BF16)
    bottom = jnp.where(even, b_box, a_box).astype(BF16)
    total = split(join(mine[:, at + b_width :]) + join(other[:, at + b_width :]))
    to = half + c_width
    halo[:, to : to + b_width] = top
    halo[:, to + b_width : to + 2 * b_width] = bottom
    halo[:, to + 2 * b_width :] = total
    boxes[:, 0:b_width] = top
    boxes[:, b_width : 2 * b_width] = bottom
    boxes[:, 2 * b_width :] = total
    coarse[...] = total


def beyond_kernel(
    n_gx, halo, near, leaf_coupling, near_part, leaf_part, scatter, leaf_base, out
):
    rows, cols, _, n_points = near_part.shape
    rank = leaf_coupling.shape[2]
    here = lax.axis_index("gx")
    parity = here % 2
    even = parity == 0
    has_halo = jnp.logical_and(here > 0, here < n_gx - 1)
    half = (cols + 2) * n_points // 2
    row_width = (cols + 4) * rank
    from_halo = []
    for u in range(rows):
        span = slice(half + u * row_width, half + (u + 1) * row_width)
        from_halo.append(jnp.where(has_halo, join(halo[:, span]), 0.0))
    strip = jnp.where(has_halo, halo[:, 0:half].astype(F32), 0.0)
    strip = jnp.concatenate([strip[:8], strip[8:]], 1).astype(BF16)
    columns = pl.ds(pl.multiple_of(parity * 6 * n_points, 6 * n_points), 3 * n_points)
    start = pl.multiple_of(jnp.where(even, 0, 14 * rank), 2 * rank)
    outers = [
        split(nt(near[parity, c, :, columns], strip[:, c * n_points : (c + 3) * n_points]).T)
        for c in range(cols)
    ]
    leaves = {}
    for c in range(cols):
        w, v = c // 2, c % 2
        window = slice(2 * w * rank, (2 * w + 6) * rank)
        even_rows = {0: from_halo[0][:, window], 1: from_halo[1][:, window]}
        odd_rows = {4: from_halo[0][:, window], 5: from_halo[1][:, window]}
        for u in range(rows):
            listed = pick_by_parity(even, even_rows, odd_rows, u, v, rank, (0, 13), (14, 27))
            leaves[u, c] = nt(listed, leaf_coupling[u, c, :, pl.ds(start, 13 * rank)])
    outers = [fold(nn(outers[c], scatter[parity, c])) for c in range(cols)]
    for u, c in leaves:
        far = fold(nn(split(leaf_part[u, c] + fold(leaves[u, c])), leaf_base[u, c]))
        out[u, c] = near_part[u, c] + far + jnp.where(parity == u, outers[c], 0.0)


def down_kernel(
    n_gx,
    n_gy,
    box_coupling,
    box_up,
    mine,
    other,
    halo,
    boxes,
    coarse,
    part,
    weights,
    box_base,
    *rest,
):
    far_parts, out = rest[:-1], rest[-1]
    rows, cols, rank, n_points = box_base.shape
    n_points = n_points // 2
    n_z = n_gx // 2
    here_x = lax.axis_index("gx")
    here_y = lax.axis_index("gy")
    parity = here_x % 2
    even = parity == 0
    z = here_x // 2
    has_up, has_down = z > 0, z < n_z - 1
    p_width = (cols + 2) * n_points
    half = p_width // 2
    row_width = (cols + 4) * rank
    c_width = 2 * row_width
    b_width = 6 * rank
    s_width = n_gy * rank

    at = p_width + c_width
    a_box, b_box = join(mine[:, at : at + b_width]), join(other[:, at : at + b_width])
    box_rows = {2: jnp.where(even, a_box, b_box), 3: jnp.where(even, b_box, a_box)}
    for u in range(2):
        start = half + c_width + u * b_width
        from_halo = join(halo[:, start : start + b_width])
        from_boxes = join(boxes[:, u * b_width : (u + 1) * b_width])
        box_rows[u] = jnp.where(has_up, jnp.where(even, from_halo, from_boxes), 0.0)
        box_rows[4 + u] = jnp.where(has_down, jnp.where(even, from_boxes, from_halo), 0.0)
    box_far = []
    for v in range(cols // 2):
        listed = jnp.where(
            even,
            pick_slots(box_rows.get, 0, v, rank, 0, 27),
            pick_slots(box_rows.get, 1, v, rank, 0, 27),
        )
        box_far.append(nt(split(listed), box_coupling[0, v]))

    lane = lax.broadcasted_iota(jnp.int32, (16, s_width), 1) // rank
    wide_gap = jnp.abs(lane - here_y) > 1
    start = half + c_width + 2 * b_width
    step = jnp.where(even, 1, -1)
    sources = [
        (z, coarse[...]),
        (lax.rem(z - step + n_z, n_z), halo[:, start:]),
        (lax.rem(z + step + n_z, n_z), boxes[:, 2 * b_width :]),
    ]
    for d, value in enumerate(far_parts):
        sources.append((lax.rem(z - (d + 2) + n_z, n_z), value[...]))
    coarse_far = None
    for place, value in sources:
        far = jnp.logical_or(wide_gap, jnp.abs(place - z) > 1)
        chosen = jnp.where(far, value.astype(F32), 0.0).astype(BF16)
        columns = pl.ds(pl.multiple_of(place * s_width, s_width), s_width)
        term = nt(chosen, weights[:, columns])
        coarse_far = term if coarse_far is None else coarse_far + term
    coarse_far = split(fold(coarse_far))

    box_down = [
        split(fold(box_far[v] + nt(coarse_far, box_up[0, v]))) for v in range(cols // 2)
    ]

    for u in range(rows):
        for c in range(cols):
            both = nn(box_down[c // 2], box_base[u, c])
            out[u, c] = part[u, c] + (fold(both[:, :n_points]) + both[:8, n_points:])


def fetching(kernel, fetch, n_in, *refs):
    count = len(fetch)
    places, arrived = refs[len(refs) - count - 1 : -1], refs[-1]
    given = list(refs[:n_in])
    copies = {}
    for k, operand in enumerate(fetch):
        copies[operand] = pltpu.make_async_copy(refs[operand], places[k], arrived.at[k])
        copies[operand].start()
        given[operand] = places[k]
    kernel(copies, *given, *refs[n_in : len(refs) - count - 1])


def call(kernel, outs, operands, scratch=(), flops=0, limit=8, hbm=(), fetch=()):
    inside = pl.BlockSpec(memory_space=pltpu.VMEM)
    outside = pl.BlockSpec(memory_space=pltpu.HBM)
    scratch = list(scratch)
    operands = [
        pltpu.with_memory_space_constraint(value, pltpu.HBM) if k in hbm + fetch else value
        for k, value in enumerate(operands)
    ]
    if fetch:
        kernel = functools.partial(
            fetching, kernel, fetch, len(operands)
        )
        scratch += [pltpu.VMEM(operands[k].shape, operands[k].dtype) for k in fetch]
        scratch.append(pltpu.SemaphoreType.DMA((len(fetch),)))
    return pl.pallas_call(
        kernel,
        out_shape=outs,
        in_specs=[outside if k in hbm + fetch else inside for k in range(len(operands))],
        out_specs=jax.tree.map(lambda _: inside, outs),
        scratch_shapes=scratch,
        cost_estimate=pl.CostEstimate(flops=flops, bytes_accessed=0, transcendentals=0),
        compiler_params=pltpu.CompilerParams(vmem_limit_bytes=limit << 20),
    )(*operands)


def body(
    n_gx,
    n_gy,
    right_sides,
    leaf_order,
    leaf_basis,
    near_blocks,
    leaf_coupling,
    leaf_transfer,
    box_coupling,
    box_transfer,
    coarse_coupling,
):
    rows, cols, n_rhs, n_points = right_sides.shape
    rank = leaf_basis.shape[2]
    n_z = n_gx // 2
    tall = 2 * n_rhs
    shape = jax.ShapeDtypeStruct

    def move(value, pairs):
        return lax.ppermute(value, "gx", pairs)

    swap = [(i, i ^ 1) for i in range(n_gx)]

    def along(by):
        return [(i, 2 * ((i // 2 + by[i % 2]) % n_z) + i % 2) for i in range(n_gx)]

    coupling_other = move(coarse_coupling, swap)
    send_width = 2 * n_points + 2 * cols * rank + 4 * rank
    pts, send = call(
        up_kernel,
        (shape((tall, cols * n_points), BF16), shape((tall, send_width), BF16)),
        (right_sides, leaf_order, leaf_basis, leaf_transfer, box_transfer),
        fetch=(1, 0, 2, 3, 4),
        flops=50000000000,
    )
    gathered = lax.all_gather(send, "gy", axis=0)
    gathered, coupling_other = lax.optimization_barrier((gathered, coupling_other))
    p_width = (cols + 2) * n_points
    c_width = 2 * (cols + 4) * rank
    b_width = 6 * rank
    s_width = n_gy * rank
    mine = call(
        functools.partial(strip_kernel, n_gy, rank, n_points, cols),
        shape((tall, p_width + c_width + b_width + s_width), BF16),
        (pts, send, gathered),
        flops=50000000000,
    )
    other = move(mine, swap)
    near_own, scatter, leaf_base, box_base = call(
        functools.partial(near_own_kernel, n_points),
        (
            shape((rows, cols, n_rhs, n_points), F32),
            shape((rows, cols, n_points, n_points), BF16),
            shape((rows, cols, rank, n_points), BF16),
            shape((rows, cols, rank, 2 * n_points), BF16),
        ),
        (mine, near_blocks, leaf_order, leaf_basis, leaf_transfer),
        flops=2 * tall * 6 * rows * cols * n_points * n_points,
        limit=8,
    )
    other, near_own = lax.optimization_barrier((other, near_own))
    halo, boxes, coarse = call(
        functools.partial(relay_kernel, rank, n_points, cols),
        (
            shape((tall, p_width // 2 + c_width + 2 * b_width + s_width), BF16),
            shape((tall, 2 * b_width + s_width), BF16),
            shape((tall, s_width), BF16),
        ),
        (mine, other),
    )
    halo_in = move(halo, along((1, -1)))
    boxes_in = move(boxes, along((-1, 1)))
    far_parts = []
    for d in range(2, n_z - 1):
        far_parts.append(move(coarse, along((d, d))))
    near_part, leaf_part, weights = call(
        mid_kernel,
        (
            shape((rows, cols, n_rhs, n_points), F32),
            shape((rows, cols, n_rhs, rank), F32),
            shape((rank, n_z * s_width), BF16),
        ),
        (
            mine,
            other,
            near_blocks,
            leaf_coupling,
            coarse_coupling,
            coupling_other,
            near_own,
            scatter,
        ),
        flops=1000000000,
        limit=8,
    )
    part = call(
        functools.partial(beyond_kernel, n_gx),
        shape((rows, cols, n_rhs, n_points), F32),
        (
            halo_in,
            near_blocks,
            leaf_coupling,
            near_part,
            leaf_part,
            scatter,
            leaf_base,
        ),
        flops=1000000000,
        limit=8,
    )
    return call(
        functools.partial(down_kernel, n_gx, n_gy),
        shape((rows, cols, n_rhs, n_points), F32),
        (
            box_coupling,
            box_transfer,
            mine,
            other,
            halo_in,
            boxes_in,
            coarse,
            part,
            weights,
            box_base,
            *far_parts,
        ),
        limit=8,
    )


def solution(mesh):
    spec = P("gx", "gy")
    return jax.shard_map(
        functools.partial(body, mesh.shape["gx"], mesh.shape["gy"]),
        mesh=mesh,
        in_specs=(spec,) * 9,
        out_specs=spec,
        check_vma=False,
    )
```

```python
import functools

import jax
import jax.numpy as jnp
from jax import lax
from jax.experimental import pallas as pl
from jax.experimental.pallas import tpu as pltpu
from jax.sharding import PartitionSpec as P


F32 = jnp.float32
BF16 = jnp.bfloat16


def nt(a, b):
    return lax.dot_general(a, b, (((1,), (1,)), ((), ())), preferred_element_type=F32)


def nn(a, b):
    return lax.dot_general(a, b, (((1,), (0,)), ((), ())), preferred_element_type=F32)


def split(x):
    hi = x.astype(BF16).astype(F32)
    return jnp.concatenate([hi, x - hi], 0).astype(BF16)


def join(y):
    half = y.shape[0] // 2
    wide = y.astype(F32)
    return wide[:half] + wide[half:]


def fold(x):
    half = x.shape[0] // 2
    return x[:half] + x[half:]


def one_hot(order_row, n_points):
    place = lax.broadcasted_iota(jnp.int32, (n_points, n_points), 0)
    return (place == order_row).astype(F32).astype(BF16)


def slot_list(u, v):
    return [
        (a, b) for a in range(6) for b in range(6) if max(abs(a - 2 - u), abs(b - 2 - v)) > 1
    ]


def pick_slots(row_of, u, v, rank, first, last):
    slots = slot_list(u, v)
    lane = None
    cache = {}

    def half(place, side):
        if place >= len(slots):
            return None
        a, b = slots[place]
        row = row_of(a)
        if row is None:
            return None
        key = (a, b // 2, b % 2 != side)
        if key not in cache:
            value = row[:, (b // 2) * 2 * rank : (b // 2 + 1) * 2 * rank]
            cache[key] = pltpu.roll(value, rank, 1) if key[2] else value
        return cache[key]

    shape = (8, 2 * rank)
    lane = lax.broadcasted_iota(jnp.int32, shape, 1)
    zero = jnp.zeros(shape, F32)
    pieces = []
    for k in range(first, last, 2):
        left, right = half(k, 0), half(k + 1, 1)
        if k + 1 == last:
            pieces.append((zero if left is None else left)[:, :rank])
        elif left is right:
            pieces.append(zero if left is None else left)
        else:
            left = zero if left is None else left
            right = zero if right is None else right
            pieces.append(jnp.where(lane < rank, left, right))
    return jnp.concatenate(pieces, 1)


def pick_by_parity(even, even_rows, odd_rows, u, v, rank, even_span, odd_span):
    return split(
        jnp.where(
            even,
            pick_slots(even_rows.get, u, v, rank, *even_span),
            pick_slots(odd_rows.get, u, v, rank, *odd_span),
        )
    )


def up_kernel(copies, rs, order, basis, leaf_up, box_up, pts, send):
    rows, cols, _, n_points = rs.shape
    rank = basis.shape[2]
    copies[1].wait()
    copies[0].wait()
    ordered = {}
    for c in range(cols):
        for u in range(rows):
            ordered[u, c] = nn(rs[u, c], one_hot(order[u, c : c + 1, :], n_points))
    copies[2].wait()
    coeff_rows = [
        [nt(ordered[u, c].astype(BF16), basis[u, c]) for c in range(cols)] for u in range(rows)
    ]
    columns = []
    for c in range(cols):
        column = jnp.concatenate([ordered[u, c] for u in range(rows)], 0).astype(BF16)
        columns.append(column)
        pts[:, c * n_points : (c + 1) * n_points] = column
    send[:, 0:n_points] = columns[0]
    send[:, n_points : 2 * n_points] = columns[-1]
    at = 2 * n_points
    wide = [jnp.concatenate(row, 1) for row in coeff_rows]
    coeffs = [split(row) for row in wide]
    for u in range(rows):
        send[:, at : at + cols * rank] = coeffs[u]
        at += cols * rank
    boxes = []
    copies[3].wait()
    copies[4].wait()
    for w in range(cols // 2):
        total = None
        for u in range(rows):
            part = nn(
                coeffs[u][:, 2 * w * rank : 2 * (w + 1) * rank],
                leaf_up[u, 2 * w : 2 * w + 2].reshape(2 * rank, rank),
            )
            total = part if total is None else total + part
        boxes.append(fold(total))
    boxes = split(jnp.concatenate(boxes, 1))
    send[:, at : at + 2 * rank] = boxes
    at += 2 * rank
    share = fold(nn(boxes, box_up[0].reshape(2 * rank, rank)))
    send[:, at : at + 2 * rank] = split(jnp.concatenate([share, share], 1))


def masked(flag, value):
    return jnp.where(flag, value.astype(F32), 0.0).astype(BF16)


def strip_kernel(n_gy, rank, n_points, cols, pts, send, gathered, out, to_pair, to_mid):
    here = lax.axis_index("gy")
    even = lax.axis_index("gx") % 2 == 0
    left = jnp.maximum(here - 1, 0)
    right = jnp.minimum(here + 1, n_gy - 1)
    has_left, has_right = here > 0, here < n_gy - 1
    first = masked(has_left, gathered[left, :, n_points : 2 * n_points])
    last = masked(has_right, gathered[right, :, 0:n_points])
    line = jnp.concatenate([first, pts[...], last], 1)
    at = (cols + 2) * n_points
    out[:, 0:at] = line
    half = at // 2
    wide = line.astype(F32)
    upper, lower = wide[:8], wide[8:]
    for row, target in (
        (jnp.where(even, upper, lower), to_pair),
        (jnp.where(even, lower, upper), to_mid),
    ):
        target[:, 0:half] = jnp.concatenate([row[:, :half], row[:, half:]], 0).astype(BF16)
    source = 2 * n_points
    width = cols * rank
    pieces = []
    for _ in range(2):
        pieces += [
            masked(has_left, gathered[left, :, source + width - 2 * rank : source + width]),
            send[:, source : source + width],
            masked(has_right, gathered[right, :, source : source + 2 * rank]),
        ]
        source += width
    coeffs = jnp.concatenate(pieces, 1)
    c_width = coeffs.shape[1]
    out[:, at : at + c_width] = coeffs
    to_pair[:, half : half + c_width] = coeffs
    pieces = [
        masked(has_left, gathered[left, :, source : source + 2 * rank]),
        send[:, source : source + 2 * rank],
        masked(has_right, gathered[right, :, source : source + 2 * rank]),
    ]
    source += 2 * rank
    lane = lax.broadcasted_iota(jnp.int32, (send.shape[0], 2 * rank), 1)
    for k in range(n_gy // 2):
        low = gathered[2 * k, :, source : source + 2 * rank].astype(F32)
        high = gathered[2 * k + 1, :, source : source + 2 * rank].astype(F32)
        pieces.append(jnp.where(lane < rank, low, high).astype(BF16))
    rest = jnp.concatenate(pieces, 1)
    out[:, at + c_width :] = rest
    to_pair[:, half + c_width :] = rest


def near_own_kernel(
    n_points, mine, near, order, basis, leaf_up, out, scatter, leaf_base, box_base
):
    rows, cols = out.shape[0], out.shape[1]
    places = jnp.concatenate([order[u] for u in range(rows)], 0).astype(F32).T
    lane = lax.broadcasted_iota(jnp.int32, (n_points, n_points), 1).astype(F32)
    wide = mine[:, 0 : (cols + 2) * n_points].astype(F32)
    top, bottom = wide[:8].astype(BF16), wide[8:].astype(BF16)
    values = {}
    for c in range(cols):
        span = slice(c * n_points, (c + 3) * n_points)
        points = jnp.concatenate([top[:, span], bottom[:, span]], 1)
        for u in range(rows):
            first = 3 * n_points * (1 - u)
            values[u, c] = nt(near[u, c, :, first : first + 6 * n_points], points)
    chosen = {}
    for c in range(cols):
        for u in range(rows):
            k = u * cols + c
            chosen[u, c] = (places[:, k : k + 1] == lane).astype(F32).astype(BF16)
            scatter[u, c] = chosen[u, c]
    moved = {}
    for u, c in chosen:
        stacked = jnp.concatenate([split(values[u, c].T), basis[u, c]], 0)
        moved[u, c] = nn(stacked, scatter[u, c])
    for u, c in chosen:
        out[u, c] = fold(moved[u, c][:16])
        moved[u, c] = moved[u, c][16:].astype(BF16)
        leaf_base[u, c] = moved[u, c]
    for u, c in chosen:
        product = nn(leaf_up[u, c].astype(F32).T.astype(BF16), moved[u, c])
        high = product.astype(BF16)
        box_base[u, c, :, 0:n_points] = high
        box_base[u, c, :, n_points:] = (product - high.astype(F32)).astype(BF16)


def mid_kernel(
    mine, other, row, near, leaf_coupling, coupling_mine, coupling_other, near_own, scatter, near_out,
    leaf_out, weights,
):
    rows, cols, _, n_points = near_own.shape
    rank = leaf_coupling.shape[2]
    parity = lax.axis_index("gx") % 2
    even = parity == 0
    p_width = (cols + 2) * n_points
    row_width = (cols + 4) * rank

    wide = row[...].astype(F32)
    rim = jnp.concatenate([wide[:8], wide[8:]], 1).astype(BF16)
    touched = 1 - parity
    outers = []
    columns = pl.ds(pl.multiple_of(touched * 6 * n_points, 6 * n_points), 3 * n_points)
    for c in range(cols):
        points = rim[:, c * n_points : (c + 3) * n_points]
        outer = nt(near[touched, c, :, columns], points).T
        outers.append(split(outer))
        near_out[parity, c] = near_own[parity, c]

    own, theirs = [], []
    for u in range(rows):
        span = slice(p_width + u * row_width, p_width + (u + 1) * row_width)
        own.append(join(mine[:, span]))
        span = slice(p_width // 2 + u * row_width, p_width // 2 + (u + 1) * row_width)
        theirs.append(join(other[:, span]))
    start = pl.multiple_of(jnp.where(even, 8 * rank, 0), 2 * rank)
    for c in range(cols):
        w, v = c // 2, c % 2
        window = slice(2 * w * rank, (2 * w + 6) * rank)
        mine_rows = {2: own[0][:, window], 3: own[1][:, window]}
        even_rows = {**mine_rows, 4: theirs[0][:, window], 5: theirs[1][:, window]}
        odd_rows = {**mine_rows, 0: theirs[0][:, window], 1: theirs[1][:, window]}
        for u in range(rows):
            listed = pick_by_parity(even, even_rows, odd_rows, u, v, rank, (8, 27), (0, 19))
            leaf_out[u, c] = fold(nt(listed, leaf_coupling[u, c, :, pl.ds(start, 19 * rank)]))

    for c in range(cols):
        outer = fold(nn(outers[c], scatter[touched, c]))
        near_out[touched, c] = near_own[touched, c] + outer
    half_width = coupling_mine.shape[-1]
    own_half = coupling_mine[0, 0].astype(F32)
    their_half = coupling_other[0, 0].astype(F32)
    weights[:, 0:half_width] = jnp.where(even, own_half, their_half).astype(BF16)
    weights[:, half_width:] = jnp.where(even, their_half, own_half).astype(BF16)


def relay_kernel(rank, n_points, cols, mine, other, halo, boxes, coarse):
    even = lax.axis_index("gx") % 2 == 0
    p_width = (cols + 2) * n_points
    c_width = 2 * (cols + 4) * rank
    b_width = 6 * rank
    to = p_width // 2 + c_width
    halo[:, 0:to] = other[:, 0:to]
    at = p_width + c_width
    a_box = mine[:, at : at + b_width].astype(F32)
    b_box = other[:, to : to + b_width].astype(F32)
    top = jnp.where(even, a_box, b_box).astype(BF16)
    bottom = jnp.where(even, b_box, a_box).astype(BF16)
    total = split(join(mine[:, at + b_width :]) + join(other[:, to + b_width :]))
    halo[:, to : to + b_width] = top
    halo[:, to + b_width : to + 2 * b_width] = bottom
    halo[:, to + 2 * b_width :] = total
    boxes[:, 0:b_width] = top
    boxes[:, b_width : 2 * b_width] = bottom
    boxes[:, 2 * b_width :] = total
    coarse[...] = total


def beyond_kernel(
    n_gx, halo, near, leaf_coupling, near_part, leaf_part, scatter, leaf_base, out
):
    rows, cols, _, n_points = near_part.shape
    rank = leaf_coupling.shape[2]
    here = lax.axis_index("gx")
    parity = here % 2
    even = parity == 0
    has_halo = jnp.logical_and(here > 0, here < n_gx - 1)
    half = (cols + 2) * n_points // 2
    row_width = (cols + 4) * rank
    from_halo = []
    for u in range(rows):
        span = slice(half + u * row_width, half + (u + 1) * row_width)
        from_halo.append(jnp.where(has_halo, join(halo[:, span]), 0.0))
    strip = jnp.where(has_halo, halo[:, 0:half].astype(F32), 0.0)
    strip = jnp.concatenate([strip[:8], strip[8:]], 1).astype(BF16)
    columns = pl.ds(pl.multiple_of(parity * 6 * n_points, 6 * n_points), 3 * n_points)
    start = pl.multiple_of(jnp.where(even, 0, 14 * rank), 2 * rank)
    outers = [
        split(nt(near[parity, c, :, columns], strip[:, c * n_points : (c + 3) * n_points]).T)
        for c in range(cols)
    ]
    leaves = {}
    for c in range(cols):
        w, v = c // 2, c % 2
        window = slice(2 * w * rank, (2 * w + 6) * rank)
        even_rows = {0: from_halo[0][:, window], 1: from_halo[1][:, window]}
        odd_rows = {4: from_halo[0][:, window], 5: from_halo[1][:, window]}
        for u in range(rows):
            listed = pick_by_parity(even, even_rows, odd_rows, u, v, rank, (0, 13), (14, 27))
            leaves[u, c] = nt(listed, leaf_coupling[u, c, :, pl.ds(start, 13 * rank)])
    outers = [fold(nn(outers[c], scatter[parity, c])) for c in range(cols)]
    for u, c in leaves:
        far = fold(nn(split(leaf_part[u, c] + fold(leaves[u, c])), leaf_base[u, c]))
        out[u, c] = near_part[u, c] + far + jnp.where(parity == u, outers[c], 0.0)


def down_kernel(
    n_gx,
    n_gy,
    box_coupling,
    box_up,
    mine,
    other,
    halo,
    boxes,
    coarse,
    part,
    weights,
    box_base,
    *rest,
):
    far_parts, out = rest[:-1], rest[-1]
    rows, cols, rank, n_points = box_base.shape
    n_points = n_points // 2
    n_z = n_gx // 2
    here_x = lax.axis_index("gx")
    here_y = lax.axis_index("gy")
    parity = here_x % 2
    even = parity == 0
    z = here_x // 2
    has_up, has_down = z > 0, z < n_z - 1
    p_width = (cols + 2) * n_points
    half = p_width // 2
    row_width = (cols + 4) * rank
    c_width = 2 * row_width
    b_width = 6 * rank
    s_width = n_gy * rank

    at = p_width + c_width
    to = half + c_width
    a_box, b_box = join(mine[:, at : at + b_width]), join(other[:, to : to + b_width])
    box_rows = {2: jnp.where(even, a_box, b_box), 3: jnp.where(even, b_box, a_box)}
    for u in range(2):
        start = half + c_width + u * b_width
        from_halo = join(halo[:, start : start + b_width])
        from_boxes = join(boxes[:, u * b_width : (u + 1) * b_width])
        box_rows[u] = jnp.where(has_up, jnp.where(even, from_halo, from_boxes), 0.0)
        box_rows[4 + u] = jnp.where(has_down, jnp.where(even, from_boxes, from_halo), 0.0)
    box_far = []
    for v in range(cols // 2):
        listed = jnp.where(
            even,
            pick_slots(box_rows.get, 0, v, rank, 0, 27),
            pick_slots(box_rows.get, 1, v, rank, 0, 27),
        )
        box_far.append(nt(split(listed), box_coupling[0, v]))

    lane = lax.broadcasted_iota(jnp.int32, (16, s_width), 1) // rank
    wide_gap = jnp.abs(lane - here_y) > 1
    start = half + c_width + 2 * b_width
    step = jnp.where(even, 1, -1)
    sources = [
        (z, coarse[...]),
        (lax.rem(z - step + n_z, n_z), halo[:, start:]),
        (lax.rem(z + step + n_z, n_z), boxes[:, 2 * b_width :]),
    ]
    for d, value in enumerate(far_parts):
        sources.append((lax.rem(z - (d + 2) + n_z, n_z), value[...]))
    coarse_far = None
    for place, value in sources:
        far = jnp.logical_or(wide_gap, jnp.abs(place - z) > 1)
        chosen = jnp.where(far, value.astype(F32), 0.0).astype(BF16)
        columns = pl.ds(pl.multiple_of(place * s_width, s_width), s_width)
        term = nt(chosen, weights[:, columns])
        coarse_far = term if coarse_far is None else coarse_far + term
    coarse_far = split(fold(coarse_far))

    box_down = [
        split(fold(box_far[v] + nt(coarse_far, box_up[0, v]))) for v in range(cols // 2)
    ]

    for u in range(rows):
        for c in range(cols):
            both = nn(box_down[c // 2], box_base[u, c])
            out[u, c] = part[u, c] + (fold(both[:, :n_points]) + both[:8, n_points:])


def fetching(kernel, fetch, n_in, *refs):
    count = len(fetch)
    places, arrived = refs[len(refs) - count - 1 : -1], refs[-1]
    given = list(refs[:n_in])
    copies = {}
    for k, operand in enumerate(fetch):
        copies[operand] = pltpu.make_async_copy(refs[operand], places[k], arrived.at[k])
        copies[operand].start()
        given[operand] = places[k]
    kernel(copies, *given, *refs[n_in : len(refs) - count - 1])


def call(kernel, outs, operands, scratch=(), flops=0, limit=8, hbm=(), fetch=()):
    inside = pl.BlockSpec(memory_space=pltpu.VMEM)
    outside = pl.BlockSpec(memory_space=pltpu.HBM)
    scratch = list(scratch)
    operands = [
        pltpu.with_memory_space_constraint(value, pltpu.HBM) if k in hbm + fetch else value
        for k, value in enumerate(operands)
    ]
    if fetch:
        kernel = functools.partial(
            fetching, kernel, fetch, len(operands)
        )
        scratch += [pltpu.VMEM(operands[k].shape, operands[k].dtype) for k in fetch]
        scratch.append(pltpu.SemaphoreType.DMA((len(fetch),)))
    return pl.pallas_call(
        kernel,
        out_shape=outs,
        in_specs=[outside if k in hbm + fetch else inside for k in range(len(operands))],
        out_specs=jax.tree.map(lambda _: inside, outs),
        scratch_shapes=scratch,
        cost_estimate=pl.CostEstimate(flops=flops, bytes_accessed=0, transcendentals=0),
        compiler_params=pltpu.CompilerParams(vmem_limit_bytes=limit << 20),
    )(*operands)


def body(
    n_gx,
    n_gy,
    right_sides,
    leaf_order,
    leaf_basis,
    near_blocks,
    leaf_coupling,
    leaf_transfer,
    box_coupling,
    box_transfer,
    coarse_coupling,
):
    rows, cols, n_rhs, n_points = right_sides.shape
    rank = leaf_basis.shape[2]
    n_z = n_gx // 2
    tall = 2 * n_rhs
    shape = jax.ShapeDtypeStruct

    def move(value, pairs):
        return lax.ppermute(value, "gx", pairs)

    swap = [(i, i ^ 1) for i in range(n_gx)]

    def along(by):
        return [(i, 2 * ((i // 2 + by[i % 2]) % n_z) + i % 2) for i in range(n_gx)]

    coupling_other = move(coarse_coupling, swap)
    send_width = 2 * n_points + 2 * cols * rank + 4 * rank
    pts, send = call(
        up_kernel,
        (shape((tall, cols * n_points), BF16), shape((tall, send_width), BF16)),
        (right_sides, leaf_order, leaf_basis, leaf_transfer, box_transfer),
        fetch=(1, 0, 2, 3, 4),
        flops=50000000000,
    )
    gathered = lax.all_gather(send, "gy", axis=0)
    gathered, coupling_other = lax.optimization_barrier((gathered, coupling_other))
    p_width = (cols + 2) * n_points
    c_width = 2 * (cols + 4) * rank
    b_width = 6 * rank
    s_width = n_gy * rank
    mine, to_pair, to_mid = call(
        functools.partial(strip_kernel, n_gy, rank, n_points, cols),
        (
            shape((tall, p_width + c_width + b_width + s_width), BF16),
            shape((tall, p_width // 2 + c_width + b_width + s_width), BF16),
            shape((tall, p_width // 2), BF16),
        ),
        (pts, send, gathered),
        flops=50000000000,
    )
    other = move(to_pair, swap)
    row = move(to_mid, swap)
    near_own, scatter, leaf_base, box_base = call(
        functools.partial(near_own_kernel, n_points),
        (
            shape((rows, cols, n_rhs, n_points), F32),
            shape((rows, cols, n_points, n_points), BF16),
            shape((rows, cols, rank, n_points), BF16),
            shape((rows, cols, rank, 2 * n_points), BF16),
        ),
        (mine, near_blocks, leaf_order, leaf_basis, leaf_transfer),
        flops=2 * tall * 6 * rows * cols * n_points * n_points,
        limit=8,
    )
    other, near_own = lax.optimization_barrier((other, near_own))
    halo, boxes, coarse = call(
        functools.partial(relay_kernel, rank, n_points, cols),
        (
            shape((tall, p_width // 2 + c_width + 2 * b_width + s_width), BF16),
            shape((tall, 2 * b_width + s_width), BF16),
            shape((tall, s_width), BF16),
        ),
        (mine, other),
    )
    halo_in = move(halo, along((1, -1)))
    boxes_in = move(boxes, along((-1, 1)))
    far_parts = []
    for d in range(2, n_z - 1):
        far_parts.append(move(coarse, along((d, d))))
    near_part, leaf_part, weights = call(
        mid_kernel,
        (
            shape((rows, cols, n_rhs, n_points), F32),
            shape((rows, cols, n_rhs, rank), F32),
            shape((rank, n_z * s_width), BF16),
        ),
        (
            mine,
            other,
            row,
            near_blocks,
            leaf_coupling,
            coarse_coupling,
            coupling_other,
            near_own,
            scatter,
        ),
        flops=1000000000,
        limit=8,
    )
    part = call(
        functools.partial(beyond_kernel, n_gx),
        shape((rows, cols, n_rhs, n_points), F32),
        (
            halo_in,
            near_blocks,
            leaf_coupling,
            near_part,
            leaf_part,
            scatter,
            leaf_base,
        ),
        flops=1000000000,
        limit=8,
    )
    return call(
        functools.partial(down_kernel, n_gx, n_gy),
        shape((rows, cols, n_rhs, n_points), F32),
        (
            box_coupling,
            box_transfer,
            mine,
            other,
            halo_in,
            boxes_in,
            coarse,
            part,
            weights,
            box_base,
            *far_parts,
        ),
        limit=8,
    )


def solution(mesh):
    spec = P("gx", "gy")
    return jax.shard_map(
        functools.partial(body, mesh.shape["gx"], mesh.shape["gy"]),
        mesh=mesh,
        in_specs=(spec,) * 9,
        out_specs=spec,
        check_vma=False,
    )
```
